256 devices in a mesh: expert: 8 (over z), tp: 32 (over x, y, core).
Axes of the slice: x: 4, y: 4, z: 8, core: 2. Of those that a mesh axis runs over, the one named last changes fastest.
Arguments:
- tokens: bfloat16 [1024, 4096], P('expert', 'tp'), may hold values from -6 to 6
- norm_gain: bfloat16 [4096], replicated, may hold values from 0.5 to 1.5
- route_logits: float32 [1024, 2], P('expert'), may hold values from -6 to 6
- expert_ids: int32 [1024, 2], P('expert'), may hold values from 0 to 7, all different within a row; in each aligned block of 128 rows (0 to 127, 128 to 255, ...) at most 64 rows name the same one
- active: int32 [1024], P('expert'), may hold values 0 or 1
- gate_weight: bfloat16 [8, 14336, 4096], P('expert', 'tp'), may hold values from -0.09375 to 0.09375
- up_weight: bfloat16 [8, 14336, 4096], P('expert', 'tp'), may hold values from -0.09375 to 0.09375
- down_weight: bfloat16 [8, 14336, 4096], P('expert', 'tp'), may hold values from -0.046875 to 0.046875
Outputs:
- mixed: bfloat16 [1024, 4096], P('expert', 'tp')
The draws below stay inside these ranges and needn't reach their ends.
Inputs may be any that keep to these rules, and one draw needn't show every extreme that they name: `expert_ids`: each token names 2 different experts. In each block of 128 consecutive token slots (the slots of one index of expert) no expert is named by more than 64 tokens, a bound that some block reaches. `active`: each entry is 0 or 1.
All inputs are finite; a program needn't handle non-finite values.
Results may differ from the reference program's by a relative error of at most 0.0025.
Values may be sent and summed in bfloat16 or wider, within the bound.
No kernel may reach another device: no remote copies, remote signals or barrier semaphores. Data moves between devices by JAX's collectives and lax.ppermute only.
A program may use at most 64 MiB of HBM per device.

```python
import math
import jax
import jax.numpy as jnp
import numpy as np
from jax import lax

D = 4096
FF = 14336
TOP = 2
WORDS_PER_GROUP = 128
EXPERTS = 8
TOKENS = 1024
CAP = 64


def with_ends(result, rng, low, high):
    extent = result.shape
    place = [jax.random.randint(jax.random.fold_in(rng, axis), (), 0, extent[axis]) for axis in range(len(extent))]
    result = result.at[tuple(place)].set(low)
    longest = extent.index(max(extent))
    place[longest] = (place[longest] + 1) % extent[longest]
    return result.at[tuple(place)].set(high)


def strengthened(array, rng, source, target, blocks, factor):
    def block_of(axis_at):
        return (jnp.arange(array.shape[axis_at]) // (array.shape[axis_at] // blocks)).reshape((-1,) + (1,) * (array.ndim - 1 - axis_at))

    first = jax.random.permutation(rng, blocks)[block_of(target)]
    other_side = (block_of(target) + blocks // 2) % blocks
    return jnp.where((block_of(source) == first) | (block_of(source) == other_side), factor * array, array)


def steps_of(own_key, dims, cuts, smallest, high):
    factor_of = 1.0
    for axis_at, blocks in cuts:
        steps = jax.random.uniform(jax.random.fold_in(jax.random.fold_in(own_key, 6), axis_at), (blocks,), jnp.float32, smallest / len(cuts), high / len(cuts))
        factor_of = factor_of * jnp.repeat(jnp.exp(steps), dims[axis_at] // blocks).reshape((-1,) + (1,) * (len(dims) - 1 - axis_at))
    return factor_of


def deal_out(rng, own, number, rows, amount, top, most, slope):
    ranking = jax.random.permutation(rng, amount)
    heavy_load, ordinary = load_shares(amount, rows * top, most, slope, True), load_shares(amount, rows * top, most, slope, False)
    places = jnp.arange(amount)

    def named(lengths, turn):
        used = int((lengths > 0).sum())
        fixed = max(1, used // 4)
        moved = fixed + (places - fixed + turn * (used - fixed)) % max(1, amount - fixed)
        return jnp.zeros((amount,), jnp.int32).at[ranking[jnp.where(places < fixed, places, moved)]].set(jnp.asarray(lengths, jnp.int32))

    lengths = jnp.where(number % 4 == 0, named(heavy_load, number // 4), named(ordinary, number - number // 4 - 1))
    mixed = jax.random.permutation(jax.random.fold_in(own, 3), amount)
    donor, receiver = mixed[0:amount // 2 * 2:2], mixed[1:amount // 2 * 2:2]
    slack = jnp.minimum(lengths[donor] - 1, most - lengths[receiver]) // 2
    slack = jnp.where((donor == ranking[0]) | (receiver == ranking[0]) | (lengths[receiver] == 0), 0, jnp.maximum(slack, 0))
    moved = jax.random.randint(jax.random.fold_in(own, 4), (amount // 2,), 0, 1 << 20) % (slack + 1)
    lengths = lengths.at[donor].add(-moved).at[receiver].add(moved)
    members = jnp.searchsorted(jnp.cumsum(lengths), jnp.arange(rows * top), side="right").astype(jnp.int32)
    grid = members.reshape(top, rows).T
    grid = grid[jax.random.permutation(jax.random.fold_in(own, 1), rows)]
    turn = jax.random.randint(jax.random.fold_in(own, 2), (rows, 1), 0, top)
    return jnp.take_along_axis(grid, (jnp.arange(top)[None, :] + turn) % top, axis=1)


def load_shares(amount, total, bound, lean, full):
    portions = [(1 << 20) // math.isqrt(standing ** lean) + 1 for standing in range(1, amount + 1)]
    largest = bound if full else min(bound, max(-(-total // amount), total * portions[0] // sum(portions)))
    least = 1 if total - largest >= amount - 1 else 0
    holding, surplus = [largest] + [least] * (amount - 1), total - largest - least * (amount - 1)
    while surplus > 0:
        candidates = [i for i in range(1, amount) if holding[i] < largest] or [i for i in range(1, amount) if holding[i] < bound]
        mass, left = sum([portions[i] for i in candidates]), surplus
        for i in candidates:
            addition = min(bound - holding[i], max(1, left * portions[i] // mass), surplus)
            holding[i] = holding[i] + addition
            surplus = surplus - addition
    return np.array(holding)


def noise(rng, dims, width, reach, pieces=(), held_as=jnp.bfloat16):
    array = width * jax.random.normal(rng, dims, jnp.float32)
    if pieces:
        array = array * steps_of(rng, dims, pieces, -0.22, 0.18)
    return jnp.clip(array, -reach, reach).astype(held_as)


def bell_draw_with(rng, shape, spread, reach, cuts, heavy, held_as=jnp.bfloat16):
    values = spread * jax.random.normal(rng, shape, jnp.float32)
    if cuts:
        values = values * steps_of(rng, shape, cuts, -0.22, 0.18)
    return jnp.clip(strengthened(values, jax.random.fold_in(rng, 3), *heavy), -reach, reach).astype(held_as)


def setup_inputs(seed: int = 0) -> dict:
    streams_of = jax.random.split(jax.random.key(seed), 9)
    tokens = bell_draw_with(streams_of[0], (TOKENS, D), 1.0, 6.0, ((0, 8), (1, 32)), (1, 0, 32, 2.75))
    norm_gain = jnp.clip(1.0 + 0.1 * jax.random.normal(streams_of[1], (D,), jnp.float32), 0.5, 1.5).astype(jnp.bfloat16)
    route_logits = noise(streams_of[2], (TOKENS, TOP), 1.0, 6.0, ((0, 8),), jnp.float32)
    expert_ids_keys = jax.random.split(jax.random.fold_in(streams_of[3], 1), TOKENS // WORDS_PER_GROUP)
    expert_ids_turns = jax.random.permutation(jax.random.fold_in(streams_of[3], 3), TOKENS // WORDS_PER_GROUP)
    expert_ids = jax.vmap(lambda own, number: deal_out(jax.random.fold_in(streams_of[3], 2), own, number, WORDS_PER_GROUP, EXPERTS, TOP, CAP, 2))(expert_ids_keys, expert_ids_turns).reshape((TOKENS, TOP))
    active = with_ends((jax.random.randint(streams_of[4], (TOKENS,), 0, 4) < 3).astype(jnp.int32), jax.random.fold_in(streams_of[4], 1), 0, 1)
    gate_weight = noise(streams_of[5], (EXPERTS, FF, D), D ** -0.5, 0.09375, ((0, 8), (1, 32)))
    up_weight = noise(streams_of[6], (EXPERTS, FF, D), D ** -0.5, 0.09375, ((0, 8), (1, 32)))
    down_weight = noise(streams_of[7], (EXPERTS, FF, D), FF ** -0.5, 0.046875, ((0, 8), (1, 32)))
    return dict(tokens=tokens, norm_gain=norm_gain, route_logits=route_logits, expert_ids=expert_ids, active=active, gate_weight=gate_weight, up_weight=up_weight, down_weight=down_weight)


epsilon = 1e-05

def reference(tokens, norm_gain, route_logits, expert_ids, active, gate_weight, up_weight, down_weight):
    widened = tokens.astype(jnp.float32)
    mean_square = lax.optimization_barrier(jnp.sum(widened * widened, axis=1, keepdims=True)) / D
    normed = (widened * lax.rsqrt(mean_square + epsilon) * norm_gain.astype(jnp.float32)).astype(jnp.bfloat16)
    route_probs = jax.nn.softmax(route_logits, axis=1) * active.astype(jnp.float32)[:, None]

    def expert_step(combined, inputs):
        specialist_number, gate_rows, up_rows, down_rows = inputs
        gate_sum = jnp.dot(normed, gate_rows.T, preferred_element_type=jnp.float32)
        up_sum = jnp.dot(normed, up_rows.T, preferred_element_type=jnp.float32)
        inner_width = (jax.nn.silu(gate_sum) * up_sum).astype(jnp.bfloat16)
        output = jnp.dot(inner_width, down_rows, preferred_element_type=jnp.float32).astype(jnp.bfloat16)
        weight = lax.optimization_barrier(jnp.sum(jnp.where(expert_ids == specialist_number, route_probs, jnp.zeros_like(route_probs)), axis=1))
        return (combined + weight[:, None] * output.astype(jnp.float32), None)
    start_value = jnp.zeros(tokens.shape, jnp.float32)
    expert_list = jnp.arange(EXPERTS, dtype=jnp.int32)
    combined, _ = lax.scan(expert_step, start_value, (expert_list, gate_weight, up_weight, down_weight))
    return combined.astype(jnp.bfloat16)
```

```python
import functools

import jax
import jax.numpy as jnp
from jax import lax
from jax.experimental import pallas as pl
from jax.experimental.pallas import tpu as pltpu
from jax.sharding import Mesh
from jax.sharding import PartitionSpec as P

TP = ("tp_0", "tp_1", "tp_2")
epsilon = 1e-05
F32, BF16 = jnp.float32, jnp.bfloat16


def shifted(array, axis, step):
    size = lax.axis_size(axis)
    return lax.ppermute(array, axis, [(i, (i + step) % size) for i in range(size)])


def seats(ids_ref, active_ref, seat_limit, experts):
    count = ids_ref.shape[0]
    eye = lax.broadcasted_iota(jnp.int32, (count, count), 0) == lax.broadcasted_iota(jnp.int32, (count, count), 1)
    live = jnp.sum(jnp.where(eye, active_ref[...], 0), axis=1, keepdims=True)
    number = lax.broadcasted_iota(jnp.int32, (count, 128), 1)
    first, second = ids_ref[:, 0:1], ids_ref[:, 1:2]
    named = ((first == number) | (second == number)) & (live > 0)
    earlier = lax.broadcasted_iota(jnp.int32, (count, count), 1) < lax.broadcasted_iota(jnp.int32, (count, count), 0)
    place = jnp.dot(earlier.astype(BF16), named.astype(BF16), preferred_element_type=F32).astype(jnp.int32)
    place = jnp.where(named, place, -1)
    columns = []
    for e in range(experts):
        spot = lax.broadcasted_iota(jnp.int32, (count, seat_limit), 1)
        columns.append(place[:, e : e + 1] == spot)
    return live, first, second, columns


def dispatch_kernel(seat_limit, experts, ids_ref, active_ref, tokens_ref, out_ref):
    _, _, _, columns = seats(ids_ref, active_ref, seat_limit, experts)
    rows = tokens_ref[...]
    for e, column in enumerate(columns):
        picked = lax.dot_general(
            column.astype(BF16), rows, (((0,), (0,)), ((), ())), preferred_element_type=F32
        )
        out_ref[e] = picked.astype(BF16)


def combine_kernel(seat_limit, experts, ids_ref, active_ref, logits_ref, arrived_ref, out_ref):
    live, first, second, columns = seats(ids_ref, active_ref, seat_limit, experts)
    logits = logits_ref[...]
    logits = logits - jnp.max(logits, axis=1, keepdims=True)
    raised = jnp.exp(logits)
    probs = raised / jnp.sum(raised, axis=1, keepdims=True) * live.astype(F32)
    total = jnp.zeros(out_ref.shape, F32)
    for k, ids in enumerate((first, second)):
        picked = jnp.zeros(out_ref.shape, F32)
        for e, column in enumerate(columns):
            hot = (column & (ids == e)).astype(BF16)
            picked = picked + jnp.dot(hot, arrived_ref[e], preferred_element_type=F32)
        total = total + probs[:, k : k + 1] * picked
    out_ref[...] = total.astype(BF16)


def expert_kernel(x_first, sizes, *refs):
    n1, n2 = sizes
    where_ref = refs[0]
    own, partner = refs[1 : 1 + n2], refs[1 + n2 : 1 + 2 * n2]
    gain_ref, gate_hbm, up_hbm, down_hbm, keep_ref, send_ref = refs[1 + 2 * n2 : 7 + 2 * n2]
    gate_ref, up_ref, down_ref, normed_ref, sems = refs[7 + 2 * n2 :]
    copies = [
        pltpu.make_async_copy(source, target, sems.at[i])
        for i, (source, target) in enumerate(
            ((gate_hbm, gate_ref), (up_hbm, up_ref), (down_hbm, down_ref))
        )
    ]
    for copy in copies:
        copy.start()
    x, y, core = where_ref[0], where_ref[1], where_ref[2]
    one, two = (x, y) if x_first else (y, x)
    rows = normed_ref.shape[0]
    width = own[0].shape[-1]

    def block(k1, k2, sign):
        a, b = lax.rem(one + sign * k1 + n1, n1), lax.rem(two + sign * k2 + n2, n2)
        return a * n2 + b if x_first else b * n1 + a

    squares = jnp.zeros((rows, width), F32)
    for pieces in (own, partner):
        for k2 in range(n2):
            for k1 in range(n1):
                value = pieces[k2][k1].astype(F32)
                squares = squares + value * value
    mean_square = jnp.sum(squares, axis=1, keepdims=True) / (2 * n1 * n2 * width)
    scale = lax.rsqrt(mean_square + epsilon)
    for pieces, parity in ((own, core), (partner, 1 - core)):
        for k2 in range(n2):
            for k1 in range(n1):
                t = block(k1, k2, -1) * 2 + parity
                value = pieces[k2][k1].astype(F32) * scale * gain_ref[t].astype(F32)
                normed_ref[:, pl.ds(pl.multiple_of(t * width, width), width)] = value.astype(BF16)
    copies[0].wait()
    copies[1].wait()
    normed = normed_ref[...]
    dims = (((1,), (1,)), ((), ()))
    gate = lax.dot_general(normed, gate_ref[...], dims, preferred_element_type=F32)
    up = lax.dot_general(normed, up_ref[...], dims, preferred_element_type=F32)
    hidden = (gate / (1.0 + jnp.exp(-gate)) * up).astype(BF16)
    copies[2].wait()
    for k1 in range(n1):
        for k2 in range(n2):
            q = block(k1, k2, 1)
            part = down_ref[:, pl.ds(pl.multiple_of(q * 2 * width, 2 * width), 2 * width)]
            both = jnp.dot(hidden, part, preferred_element_type=F32)
            low, high = both[:, :width], both[:, width:]
            keep_ref[k1, k2] = jnp.where(core == 0, low, high)
            send_ref[k1, k2] = jnp.where(core == 0, high, low)


def experts_of(x_first, where, own, partner, gains, gate, up, down):
    n2 = len(own)
    n1, rows, width = own[0].shape
    hidden, model = gate.shape
    vmem = pl.BlockSpec(memory_space=pltpu.VMEM)
    hbm = pl.BlockSpec(memory_space=pl.ANY)
    out = jax.ShapeDtypeStruct((n1, n2, rows, width), F32)
    return pl.pallas_call(
        functools.partial(expert_kernel, x_first, (n1, n2)),
        out_shape=(out, out),
        in_specs=[pl.BlockSpec(memory_space=pltpu.SMEM)] + [vmem] * (2 * n2 + 1) + [hbm] * 3,
        out_specs=(vmem, vmem),
        scratch_shapes=[
            pltpu.VMEM((hidden, model), BF16),
            pltpu.VMEM((hidden, model), BF16),
            pltpu.VMEM((hidden, model), BF16),
            pltpu.VMEM((rows, model), BF16),
            pltpu.SemaphoreType.DMA((3,)),
        ],
        compiler_params=pltpu.CompilerParams(vmem_limit_bytes=40 * 1024 * 1024),
    )(where, *own, *partner, gains, gate, up, down)


def gathered(piece, first, second):
    stack = jnp.stack([piece] + [shifted(piece, first, k) for k in range(1, lax.axis_size(first))])
    own = [stack] + [shifted(stack, second, k) for k in range(1, lax.axis_size(second))]
    return own, [shifted(a, TP[2], 1) for a in own]


def reduced(keep, send, first, second):
    total = keep + shifted(send, TP[2], 1)
    for axis in (first, second):
        parts = [shifted(total[k], axis, k) for k in range(1, lax.axis_size(axis))]
        total = sum(parts, total[0])
    return total.astype(BF16)


def local(tokens, norm_gain, route_logits, expert_ids, active, gate_weight, up_weight, down_weight):
    groups = lax.axis_size("expert")
    count, width = tokens.shape
    seat_limit = count // 2
    model = norm_gain.shape[0]
    where = jnp.stack([lax.axis_index(a) for a in TP]).astype(jnp.int32)
    gains = norm_gain.reshape(model // width, 1, width)
    active_row = active.reshape(1, count)
    sent = pl.pallas_call(
        functools.partial(dispatch_kernel, seat_limit, groups),
        out_shape=jax.ShapeDtypeStruct((groups, seat_limit, width), BF16),
    )(expert_ids, active_row, tokens)
    arriving = lax.all_to_all(sent, "expert", split_axis=0, concat_axis=0, tiled=True)
    rows = arriving.reshape(2, groups * seat_limit // 2, width)
    weights = (gate_weight[0], up_weight[0], down_weight[0])
    results = []
    for half, (first, second) in enumerate(((TP[0], TP[1]), (TP[1], TP[0]))):
        own, partner = gathered(rows[half], first, second)
        keep, send = experts_of(first == TP[0], where, own, partner, gains, *weights)
        results.append(reduced(keep, send, first, second))
    returning = jnp.stack(results).reshape(groups, seat_limit, width)
    arrived = lax.all_to_all(returning, "expert", split_axis=0, concat_axis=0, tiled=True)
    return pl.pallas_call(
        functools.partial(combine_kernel, seat_limit, groups),
        out_shape=jax.ShapeDtypeStruct((count, width), BF16),
    )(expert_ids, active_row, route_logits, arrived)


def solution(mesh):
    split = Mesh(
        mesh.devices.reshape(mesh.shape["expert"], 4, 4, 2), ("expert", "tp_0", "tp_1", "tp_2")
    )
    in_specs = (
        P("expert", TP),
        P(),
        P("expert", None),
        P("expert", None),
        P("expert"),
        P("expert", TP, None),
        P("expert", TP, None),
        P("expert", TP, None),
    )
    out_specs = P("expert", TP)
    return jax.shard_map(local, mesh=split, in_specs=in_specs, out_specs=out_specs, check_vma=False)
```

```python
import functools

import jax
import jax.numpy as jnp
from jax import lax
from jax.experimental import pallas as pl
from jax.experimental.pallas import tpu as pltpu
from jax.sharding import Mesh
from jax.sharding import PartitionSpec as P

TP = ("tp_0", "tp_1", "tp_2")
epsilon = 1e-05
F32, BF16 = jnp.float32, jnp.bfloat16


def shifted(array, axis, step):
    size = lax.axis_size(axis)
    return lax.ppermute(array, axis, [(i, (i + step) % size) for i in range(size)])


def column(row):
    count = row.shape[1]
    eye = lax.broadcasted_iota(jnp.int32, (count, count), 0) == lax.broadcasted_iota(jnp.int32, (count, count), 1)
    return jnp.sum(jnp.where(eye, row, jnp.zeros_like(row)), axis=1, keepdims=True)


def seats(ids_ref, active_ref, seat_limit, experts):
    count = ids_ref.shape[1]
    live = column(active_ref[...])
    first, second = column(ids_ref[0:1, :]), column(ids_ref[1:2, :])
    number = lax.broadcasted_iota(jnp.int32, (count, 128), 1)
    named = ((first == number) | (second == number)) & (live > 0)
    earlier = lax.broadcasted_iota(jnp.int32, (count, count), 1) < lax.broadcasted_iota(jnp.int32, (count, count), 0)
    place = jnp.dot(earlier.astype(BF16), named.astype(BF16), preferred_element_type=F32).astype(jnp.int32)
    place = jnp.where(named, place, -1)
    spot = lax.broadcasted_iota(jnp.int32, (count, seat_limit), 1)
    return live, first, second, [place[:, e : e + 1] == spot for e in range(experts)]


def dispatch_kernel(seat_limit, experts, ids_ref, active_ref, tokens_ref, out_ref):
    _, _, _, columns = seats(ids_ref, active_ref, seat_limit, experts)
    rows = tokens_ref[...]
    for e, hot in enumerate(columns):
        picked = lax.dot_general(
            hot.astype(BF16), rows, (((0,), (0,)), ((), ())), preferred_element_type=F32
        )
        out_ref[e] = picked.astype(BF16)


def combine_kernel(seat_limit, experts, ids_ref, active_ref, logits_ref, arrived_ref, out_ref):
    live, first, second, columns = seats(ids_ref, active_ref, seat_limit, experts)
    logits = logits_ref[...]
    raised = jnp.exp(logits - jnp.max(logits, axis=0, keepdims=True))
    probs = raised / jnp.sum(raised, axis=0, keepdims=True)
    total = jnp.zeros(out_ref.shape, F32)
    for k, ids in enumerate((first, second)):
        picked = jnp.zeros(out_ref.shape, F32)
        for e, hot in enumerate(columns):
            mine = (hot & (ids == e)).astype(BF16)
            picked = picked + jnp.dot(mine, arrived_ref[e], preferred_element_type=F32)
        total = total + column(probs[k : k + 1, :]) * live.astype(F32) * picked
    out_ref[...] = total.astype(BF16)


def expert_kernel(x_first, sizes, *refs):
    n1, n2 = sizes
    where_ref = refs[0]
    own, partner = refs[1 : 1 + n2], refs[1 + n2 : 1 + 2 * n2]
    gain_ref, gate_hbm, up_hbm, down_hbm, keep_ref, send_ref = refs[1 + 2 * n2 : 7 + 2 * n2]
    gate_ref, up_ref, down_ref, normed_ref, sems = refs[7 + 2 * n2 :]
    copies = [
        pltpu.make_async_copy(source, target, sems.at[i])
        for i, (source, target) in enumerate(
            ((gate_hbm, gate_ref), (up_hbm, up_ref), (down_hbm, down_ref))
        )
    ]
    for copy in copies:
        copy.start()
    x, y, core = where_ref[0], where_ref[1], where_ref[2]
    one, two = (x, y) if x_first else (y, x)
    rows = normed_ref.shape[0]
    width = own[0].shape[-1]

    def block(k1, k2, sign):
        a, b = lax.rem(one + sign * k1 + n1, n1), lax.rem(two + sign * k2 + n2, n2)
        return a * n2 + b if x_first else b * n1 + a

    squares = jnp.zeros((rows, width), F32)
    for pieces in (own, partner):
        for k2 in range(n2):
            for k1 in range(n1):
                value = pieces[k2][k1].astype(F32)
                squares = squares + value * value
    mean_square = jnp.sum(squares, axis=1, keepdims=True) / (2 * n1 * n2 * width)
    scale = lax.rsqrt(mean_square + epsilon)
    for pieces, parity in ((own, core), (partner, 1 - core)):
        for k2 in range(n2):
            for k1 in range(n1):
                t = block(k1, k2, -1) * 2 + parity
                value = pieces[k2][k1].astype(F32) * scale * gain_ref[t].astype(F32)
                normed_ref[:, pl.ds(pl.multiple_of(t * width, width), width)] = value.astype(BF16)
    copies[0].wait()
    copies[1].wait()
    normed = normed_ref[...]
    dims = (((1,), (1,)), ((), ()))
    gate = lax.dot_general(normed, gate_ref[...], dims, preferred_element_type=F32)
    up = lax.dot_general(normed, up_ref[...], dims, preferred_element_type=F32)
    hidden = (gate / (1.0 + jnp.exp(-gate)) * up).astype(BF16)
    copies[2].wait()
    for k1 in range(n1):
        for k2 in range(n2):
            q = block(k1, k2, 1)
            part = down_ref[:, pl.ds(pl.multiple_of(q * 2 * width, 2 * width), 2 * width)]
            both = jnp.dot(hidden, part, preferred_element_type=F32)
            low, high = both[:, :width], both[:, width:]
            keep_ref[k1, k2] = jnp.where(core == 0, low, high)
            send_ref[k1, k2] = jnp.where(core == 0, high, low)


def experts_of(x_first, where, own, partner, gains, gate, up, down):
    n2 = len(own)
    n1, rows, width = own[0].shape
    hidden, model = gate.shape
    vmem = pl.BlockSpec(memory_space=pltpu.VMEM)
    hbm = pl.BlockSpec(memory_space=pltpu.HBM)
    out = jax.ShapeDtypeStruct((n1, n2, rows, width), F32)
    return pl.pallas_call(
        functools.partial(expert_kernel, x_first, (n1, n2)),
        out_shape=(out, out),
        in_specs=[pl.BlockSpec(memory_space=pltpu.SMEM)] + [vmem] * (2 * n2 + 1) + [hbm] * 3,
        out_specs=(vmem, vmem),
        scratch_shapes=[
            pltpu.VMEM((hidden, model), BF16),
            pltpu.VMEM((hidden, model), BF16),
            pltpu.VMEM((hidden, model), BF16),
            pltpu.VMEM((rows, model), BF16),
            pltpu.SemaphoreType.DMA((3,)),
        ],
        compiler_params=pltpu.CompilerParams(vmem_limit_bytes=40 * 1024 * 1024),
    )(where, *own, *partner, gains, gate, up, down)


STEPS = 8
TOP = 32000.0
SPARE = 16


def scaled(blocks, refs):
    largest = functools.reduce(jnp.maximum, [jnp.abs(b) for group in blocks for b in group])
    largest = jnp.maximum(jnp.max(largest, axis=1, keepdims=True), 1e-32)
    code = jnp.ceil(STEPS * jnp.log2(largest)) + 1.0
    factor = TOP * jnp.exp2(code * (-1.0 / STEPS))
    rows, width = blocks[0][0].shape
    eye = lax.broadcasted_iota(jnp.int32, (width, width), 0) == lax.broadcasted_iota(jnp.int32, (width, width), 1)
    line = lax.broadcasted_iota(jnp.int32, (SPARE, width), 0)
    tile = jnp.zeros((SPARE, width), F32)
    for g in range(rows // width):
        part = jnp.sum(jnp.where(eye, code[g * width : (g + 1) * width], 0.0), axis=0, keepdims=True)
        tile = jnp.where(line == g, part, tile)
    for group, ref in zip(blocks, refs):
        for i, b in enumerate(group):
            ref[pl.ds(i * rows, rows), :] = jnp.round(b * factor).astype(jnp.int32).astype(jnp.int16)
        ref[pl.ds(len(group) * rows, SPARE), :] = tile.astype(jnp.int32).astype(jnp.int16)


def factors(ref, count, rows):
    tile = ref[pl.ds(count * rows, SPARE), :].astype(jnp.int32).astype(F32)
    width = tile.shape[1]
    code = jnp.concatenate([column(tile[g : g + 1, :]) for g in range(rows // width)], axis=0)
    return jnp.exp2(code * (1.0 / STEPS)) * (1.0 / TOP)


def widened(ref, i, rows):
    return ref[pl.ds(i * rows, rows), :].astype(jnp.int32).astype(F32)


def first_kernel(keep_ref, got_ref, own_ref, *out_refs):
    n1, n2, _, _ = keep_ref.shape
    for k2 in range(n2):
        own_ref[k2] = keep_ref[0, k2] + got_ref[0, k2]
    blocks = [[keep_ref[k1, k2] + got_ref[k1, k2] for k2 in range(n2)] for k1 in range(1, n1)]
    scaled(blocks, out_refs)


def second_kernel(n1, own_ref, *refs):
    got_refs, sum_ref, out_refs = refs[: n1 - 1], refs[n1 - 1], refs[n1:]
    n2, rows, _ = own_ref.shape
    by = [factors(got, n2, rows) for got in got_refs]
    totals = []
    for k2 in range(n2):
        total = own_ref[k2]
        for got, factor in zip(got_refs, by):
            total = total + widened(got, k2, rows) * factor
        totals.append(total)
    sum_ref[...] = totals[0]
    scaled([[total] for total in totals[1:]], out_refs)


def third_kernel(own_ref, *refs):
    got_refs, out_ref = refs[:-1], refs[-1]
    rows, _ = own_ref.shape
    total = own_ref[...]
    for got in got_refs:
        total = total + widened(got, 0, rows) * factors(got, 1, rows)
    out_ref[...] = total.astype(BF16)


def gathered(pieces, orders):
    got = [
        [piece] + [shifted(piece, first, k) for k in range(1, lax.axis_size(first))]
        for piece, (first, _) in zip(pieces, orders)
    ]
    got = lax.optimization_barrier(got)
    owns = []
    for parts, (_, second) in zip(got, orders):
        stack = jnp.stack(parts)
        owns.append([stack] + [shifted(stack, second, k) for k in range(1, lax.axis_size(second))])
    return [(own, [shifted(a, TP[2], 1) for a in own]) for own in owns]


def reduced(keep, send, first, second):
    n1, n2, rows, width = keep.shape
    coded = lambda blocks: jax.ShapeDtypeStruct((blocks * rows + SPARE, width), jnp.int16)
    got = shifted(send, TP[2], 1)
    own, *parts = pl.pallas_call(
        first_kernel,
        out_shape=[jax.ShapeDtypeStruct((n2, rows, width), F32)] + [coded(n2)] * (n1 - 1),
    )(keep, got)
    parts = [shifted(part, first, k + 1) for k, part in enumerate(parts)]
    own, *parts = pl.pallas_call(
        functools.partial(second_kernel, n1),
        out_shape=[jax.ShapeDtypeStruct((rows, width), F32)] + [coded(1)] * (n2 - 1),
    )(own, *parts)
    parts = [shifted(part, second, k + 1) for k, part in enumerate(parts)]
    return pl.pallas_call(third_kernel, out_shape=jax.ShapeDtypeStruct((rows, width), BF16))(own, *parts)


def local(tokens, norm_gain, route_logits, expert_ids, active, gate_weight, up_weight, down_weight):
    groups = lax.axis_size("expert")
    count, width = tokens.shape
    seat_limit = count // 2
    model = norm_gain.shape[0]
    where = jnp.stack([lax.axis_index(a) for a in TP]).astype(jnp.int32)
    gains = norm_gain.reshape(model // width, 1, width)
    active_row, ids = active.reshape(1, count), expert_ids.T
    sent = pl.pallas_call(
        functools.partial(dispatch_kernel, seat_limit, groups),
        out_shape=jax.ShapeDtypeStruct((groups, seat_limit, width), BF16),
    )(ids, active_row, tokens)
    arriving = lax.all_to_all(sent, "expert", split_axis=0, concat_axis=0, tiled=True)
    orders = ((TP[0], TP[1]), (TP[1], TP[0]))
    rows = arriving.reshape(len(orders), -1, width)
    weights = (gate_weight[0], up_weight[0], down_weight[0])
    results = []
    for (own, partner), (first, second) in zip(gathered([rows[0], rows[1]], orders), orders):
        keep, send = experts_of(first == TP[0], where, own, partner, gains, *weights)
        results.append(reduced(keep, send, first, second))
    returning = jnp.stack(results).reshape(groups, seat_limit, width)
    arrived = lax.all_to_all(returning, "expert", split_axis=0, concat_axis=0, tiled=True)
    return pl.pallas_call(
        functools.partial(combine_kernel, seat_limit, groups),
        out_shape=jax.ShapeDtypeStruct((count, width), BF16),
    )(ids, active_row, route_logits.T, arrived)


def solution(mesh):
    split = Mesh(
        mesh.devices.reshape(mesh.shape["expert"], 4, 4, 2), ("expert", "tp_0", "tp_1", "tp_2")
    )
    in_specs = (
        P("expert", TP),
        P(),
        P("expert", None),
        P("expert", None),
        P("expert"),
        P("expert", TP, None),
        P("expert", TP, None),
        P("expert", TP, None),
    )
    out_specs = P("expert", TP)
    return jax.shard_map(local, mesh=split, in_specs=in_specs, out_specs=out_specs, check_vma=False)
```

```python
import functools

import jax
import jax.numpy as jnp
from jax import lax
from jax.experimental import pallas as pl
from jax.experimental.pallas import tpu as pltpu
from jax.sharding import Mesh
from jax.sharding import PartitionSpec as P

TP = ("tp_0", "tp_1", "tp_2")
epsilon = 1e-05
F32, BF16 = jnp.float32, jnp.bfloat16
MIB = 1024 * 1024
EXPERT_MIB, LOAD_MIB = 10, 41


def shifted(array, axis, step):
    size = lax.axis_size(axis)
    return lax.ppermute(array, axis, [(i, (i + step) % size) for i in range(size)])


def column(row):
    count = row.shape[1]
    eye = lax.broadcasted_iota(jnp.int32, (count, count), 0) == lax.broadcasted_iota(jnp.int32, (count, count), 1)
    return jnp.sum(jnp.where(eye, row, jnp.zeros_like(row)), axis=1, keepdims=True)


def seats(ids_ref, active_ref, seat_limit, experts):
    count = ids_ref.shape[1]
    live = column(active_ref[...])
    first, second = column(ids_ref[0:1, :]), column(ids_ref[1:2, :])
    number = lax.broadcasted_iota(jnp.int32, (count, 128), 1)
    named = ((first == number) | (second == number)) & (live > 0)
    earlier = lax.broadcasted_iota(jnp.int32, (count, count), 1) < lax.broadcasted_iota(jnp.int32, (count, count), 0)
    place = jnp.dot(earlier.astype(BF16), named.astype(BF16), preferred_element_type=F32).astype(jnp.int32)
    place = jnp.where(named, place, -1)
    spot = lax.broadcasted_iota(jnp.int32, (count, seat_limit), 1)
    return live, first, second, [place[:, e : e + 1] == spot for e in range(experts)]


def dispatch_kernel(seat_limit, experts, ids_ref, active_ref, tokens_ref, out_ref):
    _, _, _, columns = seats(ids_ref, active_ref, seat_limit, experts)
    rows = tokens_ref[...]
    for e, hot in enumerate(columns):
        picked = lax.dot_general(
            hot.astype(BF16), rows, (((0,), (0,)), ((), ())), preferred_element_type=F32
        )
        out_ref[e] = picked.astype(BF16)


def combine_kernel(seat_limit, experts, ids_ref, active_ref, logits_ref, arrived_ref, out_ref):
    live, first, second, columns = seats(ids_ref, active_ref, seat_limit, experts)
    logits = logits_ref[...]
    raised = jnp.exp(logits - jnp.max(logits, axis=0, keepdims=True))
    probs = raised / jnp.sum(raised, axis=0, keepdims=True)
    total = jnp.zeros(out_ref.shape, F32)
    for k, ids in enumerate((first, second)):
        picked = jnp.zeros(out_ref.shape, F32)
        for e, hot in enumerate(columns):
            mine = (hot & (ids == e)).astype(BF16)
            picked = picked + jnp.dot(mine, arrived_ref[e], preferred_element_type=F32)
        total = total + column(probs[k : k + 1, :]) * live.astype(F32) * picked
    out_ref[...] = total.astype(BF16)


def expert_kernel(x_first, sizes, *refs):
    n1, n2 = sizes
    where_ref = refs[0]
    own, partner = refs[1 : 1 + n2], refs[1 + n2 : 1 + 2 * n2]
    gain_ref, gate_ref, up_ref, down_ref, keep_ref, send_ref, normed_ref = refs[1 + 2 * n2 :]
    x, y, core = where_ref[0], where_ref[1], where_ref[2]
    one, two = (x, y) if x_first else (y, x)
    rows = normed_ref.shape[0]
    width = own[0].shape[-1]

    def block(k1, k2, sign):
        a, b = lax.rem(one + sign * k1 + n1, n1), lax.rem(two + sign * k2 + n2, n2)
        return a * n2 + b if x_first else b * n1 + a

    squares = jnp.zeros((rows, width), F32)
    for pieces in (own, partner):
        for k2 in range(n2):
            for k1 in range(n1):
                value = pieces[k2][k1].astype(F32)
                squares = squares + value * value
    mean_square = jnp.sum(squares, axis=1, keepdims=True) / (2 * n1 * n2 * width)
    scale = lax.rsqrt(mean_square + epsilon)
    for pieces, parity in ((own, core), (partner, 1 - core)):
        for k2 in range(n2):
            for k1 in range(n1):
                t = block(k1, k2, -1) * 2 + parity
                value = pieces[k2][k1].astype(F32) * scale * gain_ref[t].astype(F32)
                normed_ref[:, pl.ds(pl.multiple_of(t * width, width), width)] = value.astype(BF16)
    normed = normed_ref[...]
    dims = (((1,), (1,)), ((), ()))
    gate = lax.dot_general(normed, gate_ref[...], dims, preferred_element_type=F32)
    up = lax.dot_general(normed, up_ref[...], dims, preferred_element_type=F32)
    hidden = (gate / (1.0 + jnp.exp(-gate)) * up).astype(BF16)
    for k1 in range(n1):
        for k2 in range(n2):
            q = block(k1, k2, 1)
            part = down_ref[:, pl.ds(pl.multiple_of(q * 2 * width, 2 * width), 2 * width)]
            both = jnp.dot(hidden, part, preferred_element_type=F32)
            low, high = both[:, :width], both[:, width:]
            keep_ref[k1, k2] = jnp.where(core == 0, low, high)
            send_ref[k1, k2] = jnp.where(core == 0, high, low)


def load_kernel(_, *refs):
    sources, targets, sems = refs[:3], refs[3:6], refs[6]
    copies = [pltpu.make_async_copy(a, b, sems.at[i]) for i, (a, b) in enumerate(zip(sources, targets))]
    for copy in copies:
        copy.start()
    for copy in copies:
        copy.wait()


def loaded(after, weights):
    hbm = pl.BlockSpec(memory_space=pltpu.HBM)
    return pl.pallas_call(
        load_kernel,
        out_shape=[jax.ShapeDtypeStruct(w.shape, w.dtype) for w in weights],
        in_specs=[hbm] * (1 + len(weights)),
        out_specs=[pl.BlockSpec(memory_space=pltpu.VMEM)] * len(weights),
        scratch_shapes=[pltpu.SemaphoreType.DMA((len(weights),))],
        compiler_params=pltpu.CompilerParams(vmem_limit_bytes=LOAD_MIB * MIB),
        cost_estimate=pl.CostEstimate(flops=1500000000, transcendentals=0, bytes_accessed=0),
    )(after, *weights)


def experts_of(x_first, where, own, partner, gains, gate, up, down):
    n2 = len(own)
    n1, rows, width = own[0].shape
    model = gate.shape[1]
    vmem = pl.BlockSpec(memory_space=pltpu.VMEM)
    out = jax.ShapeDtypeStruct((n1, n2, rows, width), F32)
    return pl.pallas_call(
        functools.partial(expert_kernel, x_first, (n1, n2)),
        out_shape=(out, out),
        in_specs=[pl.BlockSpec(memory_space=pltpu.SMEM)] + [vmem] * (2 * n2 + 4),
        out_specs=(vmem, vmem),
        scratch_shapes=[pltpu.VMEM((rows, model), BF16)],
        compiler_params=pltpu.CompilerParams(vmem_limit_bytes=EXPERT_MIB * MIB),
        cost_estimate=pl.CostEstimate(flops=3000000000, transcendentals=0, bytes_accessed=0),
    )(where, *own, *partner, gains, gate, up, down)


STEPS = 8
TOP = 32000.0
SPARE = 16


def scaled(blocks, refs):
    largest = functools.reduce(jnp.maximum, [jnp.abs(b) for group in blocks for b in group])
    largest = jnp.maximum(jnp.max(largest, axis=1, keepdims=True), 1e-32)
    code = jnp.ceil(STEPS * jnp.log2(largest)) + 1.0
    factor = TOP * jnp.exp2(code * (-1.0 / STEPS))
    rows, width = blocks[0][0].shape
    eye = lax.broadcasted_iota(jnp.int32, (width, width), 0) == lax.broadcasted_iota(jnp.int32, (width, width), 1)
    line = lax.broadcasted_iota(jnp.int32, (SPARE, width), 0)
    tile = jnp.zeros((SPARE, width), F32)
    for g in range(rows // width):
        part = jnp.sum(jnp.where(eye, code[g * width : (g + 1) * width], 0.0), axis=0, keepdims=True)
        tile = jnp.where(line == g, part, tile)
    for group, ref in zip(blocks, refs):
        for i, b in enumerate(group):
            ref[pl.ds(i * rows, rows), :] = jnp.round(b * factor).astype(jnp.int32).astype(jnp.int16)
        ref[pl.ds(len(group) * rows, SPARE), :] = tile.astype(jnp.int32).astype(jnp.int16)


def factors(ref, count, rows):
    tile = ref[pl.ds(count * rows, SPARE), :].astype(jnp.int32).astype(F32)
    width = tile.shape[1]
    code = jnp.concatenate([column(tile[g : g + 1, :]) for g in range(rows // width)], axis=0)
    return jnp.exp2(code * (1.0 / STEPS)) * (1.0 / TOP)


def widened(ref, i, rows):
    return ref[pl.ds(i * rows, rows), :].astype(jnp.int32).astype(F32)


def first_kernel(keep_ref, got_ref, own_ref, *out_refs):
    n1, n2, _, _ = keep_ref.shape
    for k2 in range(n2):
        own_ref[k2] = keep_ref[0, k2] + got_ref[0, k2]
    blocks = [[keep_ref[k1, k2] + got_ref[k1, k2] for k2 in range(n2)] for k1 in range(1, n1)]
    scaled(blocks, out_refs)


def second_kernel(n1, own_ref, *refs):
    got_refs, sum_ref, out_refs = refs[: n1 - 1], refs[n1 - 1], refs[n1:]
    n2, rows, _ = own_ref.shape
    by = [factors(got, n2, rows) for got in got_refs]
    totals = []
    for k2 in range(n2):
        total = own_ref[k2]
        for got, factor in zip(got_refs, by):
            total = total + widened(got, k2, rows) * factor
        totals.append(total)
    sum_ref[...] = totals[0]
    scaled([[total] for total in totals[1:]], out_refs)


def third_kernel(own_ref, *refs):
    got_refs, out_ref = refs[:-1], refs[-1]
    rows, _ = own_ref.shape
    total = own_ref[...]
    for got in got_refs:
        total = total + widened(got, 0, rows) * factors(got, 1, rows)
    out_ref[...] = total.astype(BF16)


def gathered(pieces, orders):
    got = [
        [piece] + [shifted(piece, first, k) for k in range(1, lax.axis_size(first))]
        for piece, (first, _) in zip(pieces, orders)
    ]
    got = lax.optimization_barrier(got)
    owns = []
    for parts, (_, second) in zip(got, orders):
        stack = jnp.stack(parts)
        owns.append([stack] + [shifted(stack, second, k) for k in range(1, lax.axis_size(second))])
    return [(own, [shifted(a, TP[2], 1) for a in own]) for own in owns]


def reduced(keep, send, first, second):
    n1, n2, rows, width = keep.shape
    coded = lambda blocks: jax.ShapeDtypeStruct((blocks * rows + SPARE, width), jnp.int16)
    got = shifted(send, TP[2], 1)
    own, *parts = pl.pallas_call(
        first_kernel,
        out_shape=[jax.ShapeDtypeStruct((n2, rows, width), F32)] + [coded(n2)] * (n1 - 1),
        compiler_params=pltpu.CompilerParams(vmem_limit_bytes=8 * MIB),
    )(keep, got)
    parts = [shifted(part, first, k + 1) for k, part in enumerate(parts)]
    own, *parts = pl.pallas_call(
        functools.partial(second_kernel, n1),
        out_shape=[jax.ShapeDtypeStruct((rows, width), F32)] + [coded(1)] * (n2 - 1),
        compiler_params=pltpu.CompilerParams(vmem_limit_bytes=4 * MIB),
    )(own, *parts)
    parts = [shifted(part, second, k + 1) for k, part in enumerate(parts)]
    return pl.pallas_call(
        third_kernel,
        out_shape=jax.ShapeDtypeStruct((rows, width), BF16),
        compiler_params=pltpu.CompilerParams(vmem_limit_bytes=2 * MIB),
    )(own, *parts)


def local(tokens, norm_gain, route_logits, expert_ids, active, gate_weight, up_weight, down_weight):
    groups = lax.axis_size("expert")
    count, width = tokens.shape
    seat_limit = count // 2
    model = norm_gain.shape[0]
    where = jnp.stack([lax.axis_index(a) for a in TP]).astype(jnp.int32)
    gains = norm_gain.reshape(model // width, 1, width)
    active_row, ids = active.reshape(1, count), expert_ids.T
    sent = pl.pallas_call(
        functools.partial(dispatch_kernel, seat_limit, groups),
        out_shape=jax.ShapeDtypeStruct((groups, seat_limit, width), BF16),
        compiler_params=pltpu.CompilerParams(vmem_limit_bytes=2 * MIB),
    )(ids, active_row, tokens)
    arriving = lax.all_to_all(sent, "expert", split_axis=0, concat_axis=0, tiled=True)
    orders = ((TP[0], TP[1]), (TP[1], TP[0]))
    rows = arriving.reshape(len(orders), -1, width)
    weights = loaded(rows[0], (gate_weight[0], up_weight[0], down_weight[0]))
    results = []
    for (own, partner), (first, second) in zip(gathered([rows[0], rows[1]], orders), orders):
        keep, send = experts_of(first == TP[0], where, own, partner, gains, *weights)
        results.append(reduced(keep, send, first, second))
    returning = jnp.stack(results).reshape(groups, seat_limit, width)
    arrived = lax.all_to_all(returning, "expert", split_axis=0, concat_axis=0, tiled=True)
    return pl.pallas_call(
        functools.partial(combine_kernel, seat_limit, groups),
        out_shape=jax.ShapeDtypeStruct((count, width), BF16),
        compiler_params=pltpu.CompilerParams(vmem_limit_bytes=2 * MIB),
    )(ids, active_row, route_logits.T, arrived)


def solution(mesh):
    split = Mesh(
        mesh.devices.reshape(mesh.shape["expert"], 4, 4, 2), ("expert", "tp_0", "tp_1", "tp_2")
    )
    in_specs = (
        P("expert", TP),
        P(),
        P("expert", None),
        P("expert", None),
        P("expert"),
        P("expert", TP, None),
        P("expert", TP, None),
        P("expert", TP, None),
    )
    out_specs = P("expert", TP)
    return jax.shard_map(local, mesh=split, in_specs=in_specs, out_specs=out_specs, check_vma=False)
```

```python
import functools

import jax
import jax.numpy as jnp
from jax import lax
from jax.experimental import pallas as pl
from jax.experimental.pallas import tpu as pltpu
from jax.sharding import Mesh
from jax.sharding import PartitionSpec as P

TP = ("tp_0", "tp_1", "tp_2")
epsilon = 1e-05
F32, BF16 = jnp.float32, jnp.bfloat16
MIB = 1024 * 1024
CHUNKS = 2
LOAD_MIB = 41


def moved(array, target):
    nx, ny, cores = (lax.axis_size(a) for a in TP)
    flat = lambda x, y, core: ((x % nx) * ny + y % ny) * cores + core
    pairs = [
        (flat(x, y, core), flat(*target(x, y, core)))
        for x in range(nx)
        for y in range(ny)
        for core in range(cores)
    ]
    return lax.ppermute(array, TP, pairs)


def along(array, stage, step):
    def target(x, y, core):
        return (x + step, y, core) if core == stage else (x, y + step, core)

    return moved(array, target)


def swapped(array):
    return moved(array, lambda x, y, core: (x, y, 1 - core))


def column(row):
    count = row.shape[1]
    eye = lax.broadcasted_iota(jnp.int32, (count, count), 0) == lax.broadcasted_iota(jnp.int32, (count, count), 1)
    return jnp.sum(jnp.where(eye, row, jnp.zeros_like(row)), axis=1, keepdims=True)


def seats(ids_ref, active_ref, seat_limit, experts):
    count = ids_ref.shape[1]
    live = column(active_ref[...])
    first, second = column(ids_ref[0:1, :]), column(ids_ref[1:2, :])
    number = lax.broadcasted_iota(jnp.int32, (count, 128), 1)
    named = ((first == number) | (second == number)) & (live > 0)
    earlier = lax.broadcasted_iota(jnp.int32, (count, count), 1) < lax.broadcasted_iota(jnp.int32, (count, count), 0)
    place = jnp.dot(earlier.astype(BF16), named.astype(BF16), preferred_element_type=F32).astype(jnp.int32)
    place = jnp.where(named, place, -1)
    spot = lax.broadcasted_iota(jnp.int32, (count, seat_limit), 1)
    return live, first, second, [place[:, e : e + 1] == spot for e in range(experts)]


def dispatch_kernel(seat_limit, experts, ids_ref, active_ref, tokens_ref, out_ref):
    _, _, _, columns = seats(ids_ref, active_ref, seat_limit, experts)
    rows = tokens_ref[...]
    for e, hot in enumerate(columns):
        picked = lax.dot_general(
            hot.astype(BF16), rows, (((0,), (0,)), ((), ())), preferred_element_type=F32
        )
        out_ref[e] = picked.astype(BF16)


def combine_kernel(seat_limit, experts, ids_ref, active_ref, logits_ref, arrived_ref, out_ref):
    live, first, second, columns = seats(ids_ref, active_ref, seat_limit, experts)
    logits = logits_ref[...]
    raised = jnp.exp(logits - jnp.max(logits, axis=0, keepdims=True))
    probs = raised / jnp.sum(raised, axis=0, keepdims=True)
    total = jnp.zeros(out_ref.shape, F32)
    for k, ids in enumerate((first, second)):
        picked = jnp.zeros(out_ref.shape, F32)
        for e, hot in enumerate(columns):
            mine = (hot & (ids == e)).astype(BF16)
            picked = picked + jnp.dot(mine, arrived_ref[e], preferred_element_type=F32)
        total = total + column(probs[k : k + 1, :]) * live.astype(F32) * picked
    out_ref[...] = total.astype(BF16)


def expert_kernel(n, where_ref, *refs):
    own, partner = refs[:n], refs[n : 2 * n]
    gain_ref, gate_ref, up_ref, down_ref, keep_ref, send_ref, normed_ref = refs[2 * n :]
    x, y, core = where_ref[0], where_ref[1], where_ref[2]
    rows = normed_ref.shape[0]
    width = own[0].shape[-1]
    squares = jnp.zeros((rows, width), F32)
    for pieces in (own, partner):
        for k2 in range(n):
            for k1 in range(n):
                value = pieces[k2][k1].astype(F32)
                squares = squares + value * value
    mean_square = jnp.sum(squares, axis=1, keepdims=True) / (2 * n * n * width)
    scale = lax.rsqrt(mean_square + epsilon)
    for pieces, parity in ((own, core), (partner, 1 - core)):
        for k2 in range(n):
            for k1 in range(n):
                at_x = lax.rem(x - jnp.where(parity == 0, k1, k2) + n, n)
                at_y = lax.rem(y - jnp.where(parity == 0, k2, k1) + n, n)
                t = (at_x * n + at_y) * 2 + parity
                value = pieces[k2][k1].astype(F32) * scale * gain_ref[t].astype(F32)
                normed_ref[:, pl.ds(pl.multiple_of(t * width, width), width)] = value.astype(BF16)
    normed = normed_ref[...]
    dims = (((1,), (1,)), ((), ()))
    gate = lax.dot_general(normed, gate_ref[...], dims, preferred_element_type=F32)
    up = lax.dot_general(normed, up_ref[...], dims, preferred_element_type=F32)
    hidden = (gate / (1.0 + jnp.exp(-gate)) * up).astype(BF16)
    for dx in range(n):
        for dy in range(n):
            q = lax.rem(x + dx, n) * n + lax.rem(y + dy, n)
            part = down_ref[:, pl.ds(pl.multiple_of(q * 2 * width, 2 * width), 2 * width)]
            both = jnp.dot(hidden, part, preferred_element_type=F32)
            low, high = both[:, :width], both[:, width:]
            one, two = jnp.where(core == 0, dx, dy), jnp.where(core == 0, dy, dx)
            keep_ref[one, two] = jnp.where(core == 0, low, high)
            send_ref[two, one] = jnp.where(core == 0, high, low)


def load_kernel(_, *refs):
    sources, targets, sems = refs[:3], refs[3:6], refs[6]
    copies = [pltpu.make_async_copy(a, b, sems.at[i]) for i, (a, b) in enumerate(zip(sources, targets))]
    for copy in copies:
        copy.start()
    for copy in copies:
        copy.wait()


def loaded(after, weights):
    hbm = pl.BlockSpec(memory_space=pltpu.HBM)
    return pl.pallas_call(
        load_kernel,
        out_shape=[jax.ShapeDtypeStruct(w.shape, w.dtype) for w in weights],
        in_specs=[hbm] * (1 + len(weights)),
        out_specs=[pl.BlockSpec(memory_space=pltpu.VMEM)] * len(weights),
        scratch_shapes=[pltpu.SemaphoreType.DMA((len(weights),))],
        compiler_params=pltpu.CompilerParams(vmem_limit_bytes=LOAD_MIB * MIB),
        cost_estimate=pl.CostEstimate(flops=1500000000, transcendentals=0, bytes_accessed=0),
    )(after, *weights)


def experts_of(where, own, partner, gains, gate, up, down):
    n = len(own)
    _, rows, width = own[0].shape
    model = gate.shape[1]
    vmem = pl.BlockSpec(memory_space=pltpu.VMEM)
    out = jax.ShapeDtypeStruct((n, n, rows, width), F32)
    return pl.pallas_call(
        functools.partial(expert_kernel, n),
        out_shape=(out, out),
        in_specs=[pl.BlockSpec(memory_space=pltpu.SMEM)] + [vmem] * (2 * n + 4),
        out_specs=(vmem, vmem),
        scratch_shapes=[pltpu.VMEM((rows, model), BF16)],
        compiler_params=pltpu.CompilerParams(vmem_limit_bytes=10 * MIB),
        cost_estimate=pl.CostEstimate(flops=3000000000, transcendentals=0, bytes_accessed=0),
    )(where, *own, *partner, gains, gate, up, down)


STEPS = 8
TOP = 32000.0
SPARE = 16


def scaled(blocks, refs):
    largest = functools.reduce(jnp.maximum, [jnp.abs(b) for group in blocks for b in group])
    largest = jnp.maximum(jnp.max(largest, axis=1, keepdims=True), 1e-32)
    code = jnp.ceil(STEPS * jnp.log2(largest)) + 1.0
    factor = TOP * jnp.exp2(code * (-1.0 / STEPS))
    rows, width = blocks[0][0].shape
    eye = lax.broadcasted_iota(jnp.int32, (width, width), 0) == lax.broadcasted_iota(jnp.int32, (width, width), 1)
    line = lax.broadcasted_iota(jnp.int32, (SPARE, width), 0)
    tile = jnp.zeros((SPARE, width), F32)
    for g in range(rows // width):
        part = jnp.sum(jnp.where(eye, code[g * width : (g + 1) * width], 0.0), axis=0, keepdims=True)
        tile = jnp.where(line == g, part, tile)
    for group, ref in zip(blocks, refs):
        for i, b in enumerate(group):
            ref[pl.ds(i * rows, rows), :] = jnp.round(b * factor).astype(jnp.int32).astype(jnp.int16)
        ref[pl.ds(len(group) * rows, SPARE), :] = tile.astype(jnp.int32).astype(jnp.int16)


def factors(ref, count, rows):
    tile = ref[pl.ds(count * rows, SPARE), :].astype(jnp.int32).astype(F32)
    width = tile.shape[1]
    code = jnp.concatenate([column(tile[g : g + 1, :]) for g in range(rows // width)], axis=0)
    return jnp.exp2(code * (1.0 / STEPS)) * (1.0 / TOP)


def widened(ref, i, rows):
    return ref[pl.ds(i * rows, rows), :].astype(jnp.int32).astype(F32)


def first_kernel(keep_ref, got_ref, own_ref, *out_refs):
    n = keep_ref.shape[0]
    for k2 in range(n):
        own_ref[k2] = keep_ref[0, k2] + got_ref[0, k2]
    blocks = [[keep_ref[k1, k2] + got_ref[k1, k2] for k2 in range(n)] for k1 in range(1, n)]
    scaled(blocks, out_refs)


def second_kernel(chunks, *refs):
    ins, sum_ref, out_refs = refs[: 4 * chunks], refs[4 * chunks], refs[4 * chunks + 1 :]
    n, rows, _ = ins[0].shape
    totals = []
    for chunk in range(chunks):
        own_ref, *got_refs = ins[4 * chunk : 4 * chunk + 4]
        by = [factors(got, n, rows) for got in got_refs]
        totals.append([])
        for k2 in range(n):
            total = own_ref[k2]
            for got, factor in zip(got_refs, by):
                total = total + widened(got, k2, rows) * factor
            totals[-1].append(total)
    totals = [jnp.concatenate(parts, axis=0) for parts in zip(*totals)]
    sum_ref[...] = totals[0]
    scaled([[total] for total in totals[1:]], out_refs)


def third_kernel(own_ref, *refs):
    got_refs, out_ref = refs[:-1], refs[-1]
    rows, _ = own_ref.shape
    total = own_ref[...]
    for got in got_refs:
        total = total + widened(got, 0, rows) * factors(got, 1, rows)
    out_ref[...] = total.astype(BF16)


def coded(blocks, rows, width):
    return jax.ShapeDtypeStruct((blocks * rows + SPARE, width), jnp.int16)


def started(keep, send):
    n, _, rows, width = keep.shape
    own, *parts = pl.pallas_call(
        first_kernel,
        out_shape=[jax.ShapeDtypeStruct((n, rows, width), F32)] + [coded(n, rows, width)] * (n - 1),
        compiler_params=pltpu.CompilerParams(vmem_limit_bytes=8 * MIB),
    )(keep, swapped(send))
    return [own] + [along(part, 0, k + 1) for k, part in enumerate(parts)]


def finished(chunks):
    n, rows, width = chunks[0][0].shape
    rows = rows * len(chunks)
    own, *parts = pl.pallas_call(
        functools.partial(second_kernel, len(chunks)),
        out_shape=[jax.ShapeDtypeStruct((rows, width), F32)] + [coded(1, rows, width)] * (n - 1),
        compiler_params=pltpu.CompilerParams(vmem_limit_bytes=4 * MIB),
    )(*[a for chunk in chunks for a in chunk])
    parts = [along(part, 1, k + 1) for k, part in enumerate(parts)]
    return pl.pallas_call(
        third_kernel,
        out_shape=jax.ShapeDtypeStruct((rows, width), BF16),
        compiler_params=pltpu.CompilerParams(vmem_limit_bytes=2 * MIB),
    )(own, *parts)


def local(tokens, norm_gain, route_logits, expert_ids, active, gate_weight, up_weight, down_weight):
    groups = lax.axis_size("expert")
    count, width = tokens.shape
    seat_limit = count // 2
    model = norm_gain.shape[0]
    where = jnp.stack([lax.axis_index(a) for a in TP]).astype(jnp.int32)
    gains = norm_gain.reshape(model // width, 1, width)
    active_row, ids = active.reshape(1, count), expert_ids.T
    sent = pl.pallas_call(
        functools.partial(dispatch_kernel, seat_limit, groups),
        out_shape=jax.ShapeDtypeStruct((groups, seat_limit, width), BF16),
        compiler_params=pltpu.CompilerParams(vmem_limit_bytes=60 * MIB),
    )(ids, active_row, tokens)
    arriving = lax.all_to_all(sent, "expert", split_axis=0, concat_axis=0, tiled=True)
    n = lax.axis_size(TP[0])
    rows = arriving.reshape(CHUNKS, -1, width)
    first = [rows] + [along(rows, 0, k) for k in range(1, n)]
    weights = loaded(rows, (gate_weight[0], up_weight[0], down_weight[0]))
    owns = []
    for chunk in range(CHUNKS):
        stack = jnp.stack([a[chunk] for a in first])
        owns.append([stack] + [along(stack, 1, k) for k in range(1, n)])
    chunks = []
    for own in owns:
        keep, send = experts_of(where, own, [swapped(a) for a in own], gains, *weights)
        chunks.append(started(keep, send))
    returning = finished(chunks).reshape(groups, seat_limit, width)
    arrived = lax.all_to_all(returning, "expert", split_axis=0, concat_axis=0, tiled=True)
    return pl.pallas_call(
        functools.partial(combine_kernel, seat_limit, groups),
        out_shape=jax.ShapeDtypeStruct((count, width), BF16),
        compiler_params=pltpu.CompilerParams(vmem_limit_bytes=2 * MIB),
    )(ids, active_row, route_logits.T, arrived)


def solution(mesh):
    split = Mesh(
        mesh.devices.reshape(mesh.shape["expert"], 4, 4, 2), ("expert", "tp_0", "tp_1", "tp_2")
    )
    in_specs = (
        P("expert", TP),
        P(),
        P("expert", None),
        P("expert", None),
        P("expert"),
        P("expert", TP, None),
        P("expert", TP, None),
        P("expert", TP, None),
    )
    out_specs = P("expert", TP)
    return jax.shard_map(local, mesh=split, in_specs=in_specs, out_specs=out_specs, check_vma=False)
```

```python
import functools

import jax
import jax.numpy as jnp
from jax import lax
from jax.experimental import pallas as pl
from jax.experimental.pallas import tpu as pltpu
from jax.sharding import Mesh
from jax.sharding import PartitionSpec as P


TP = ("tp_0", "tp_1", "tp_2")
epsilon = 1e-05
F32, BF16 = jnp.float32, jnp.bfloat16
MIB = 1024 * 1024
CHUNKS = 2
LOAD_MIB = 41


def moved(array, target):
    nx, ny, cores = (lax.axis_size(a) for a in TP)
    flat = lambda x, y, core: ((x % nx) * ny + y % ny) * cores + core
    pairs = [
        (flat(x, y, core), flat(*target(x, y, core)))
        for x in range(nx)
        for y in range(ny)
        for core in range(cores)
    ]
    return lax.ppermute(array, TP, pairs)


def along(array, stage, step):
    def target(x, y, core):
        return (x + step, y, core) if core == stage else (x, y + step, core)

    return moved(array, target)


def swapped(array):
    return moved(array, lambda x, y, core: (x, y, 1 - core))


def column(row):
    count = row.shape[1]
    eye = lax.broadcasted_iota(jnp.int32, (count, count), 0) == lax.broadcasted_iota(jnp.int32, (count, count), 1)
    return jnp.sum(jnp.where(eye, row, jnp.zeros_like(row)), axis=1, keepdims=True)


def seats(ids_ref, active_ref, seat_limit, experts):
    count = ids_ref.shape[1]
    live = column(active_ref[...])
    first, second = column(ids_ref[0:1, :]), column(ids_ref[1:2, :])
    number = lax.broadcasted_iota(jnp.int32, (count, 128), 1)
    named = ((first == number) | (second == number)) & (live > 0)
    earlier = lax.broadcasted_iota(jnp.int32, (count, count), 1) < lax.broadcasted_iota(jnp.int32, (count, count), 0)
    place = jnp.dot(earlier.astype(BF16), named.astype(BF16), preferred_element_type=F32).astype(jnp.int32)
    place = jnp.where(named, place, -1)
    spot = lax.broadcasted_iota(jnp.int32, (count, seat_limit), 1)
    return live, first, second, [place[:, e : e + 1] == spot for e in range(experts)]


def dispatch_kernel(seat_limit, experts, ids_ref, active_ref, tokens_ref, out_ref):
    _, _, _, columns = seats(ids_ref, active_ref, seat_limit, experts)
    rows = tokens_ref[...]
    for e, hot in enumerate(columns):
        picked = lax.dot_general(
            hot.astype(BF16), rows, (((0,), (0,)), ((), ())), preferred_element_type=F32
        )
        out_ref[e] = picked.astype(BF16)


def combine_kernel(seat_limit, experts, ids_ref, active_ref, logits_ref, arrived_ref, out_ref):
    live, first, second, columns = seats(ids_ref, active_ref, seat_limit, experts)
    logits = logits_ref[...]
    raised = jnp.exp(logits - jnp.max(logits, axis=0, keepdims=True))
    probs = raised / jnp.sum(raised, axis=0, keepdims=True)
    total = jnp.zeros(out_ref.shape, F32)
    for k, ids in enumerate((first, second)):
        picked = jnp.zeros(out_ref.shape, F32)
        for e, hot in enumerate(columns):
            mine = (hot & (ids == e)).astype(BF16)
            picked = picked + jnp.dot(mine, arrived_ref[e], preferred_element_type=F32)
        total = total + column(probs[k : k + 1, :]) * live.astype(F32) * picked
    out_ref[...] = total.astype(BF16)


def expert_kernel(n, where_ref, *refs):
    own, partner = refs[:n], refs[n : 2 * n]
    gain_ref, gate_ref, up_ref, down_ref, keep_ref, send_ref, normed_ref = refs[2 * n :]
    x, y, core = where_ref[0], where_ref[1], where_ref[2]
    rows = normed_ref.shape[0]
    width = own[0].shape[-1]
    squares = jnp.zeros((rows, width), F32)
    for pieces in (own, partner):
        for k2 in range(n):
            for k1 in range(n):
                value = pieces[k2][k1].astype(F32)
                squares = squares + value * value
    mean_square = jnp.sum(squares, axis=1, keepdims=True) / (2 * n * n * width)
    scale = lax.rsqrt(mean_square + epsilon)
    for pieces, parity in ((own, core), (partner, 1 - core)):
        for k2 in range(n):
            for k1 in range(n):
                at_x = lax.rem(x - jnp.where(parity == 0, k1, k2) + n, n)
                at_y = lax.rem(y - jnp.where(parity == 0, k2, k1) + n, n)
                t = (at_x * n + at_y) * 2 + parity
                value = pieces[k2][k1].astype(F32) * scale * gain_ref[:, pl.ds(pl.multiple_of(t * width, width), width)].astype(F32)
                normed_ref[:, pl.ds(pl.multiple_of(t * width, width), width)] = value.astype(BF16)
    normed = normed_ref[...]
    dims = (((1,), (1,)), ((), ()))
    gate = lax.dot_general(normed, gate_ref[...], dims, preferred_element_type=F32)
    up = lax.dot_general(normed, up_ref[...], dims, preferred_element_type=F32)
    hidden = (gate / (1.0 + jnp.exp(-gate)) * up).astype(BF16)
    for dx in range(n):
        for dy in range(n):
            q = lax.rem(x + dx, n) * n + lax.rem(y + dy, n)
            part = down_ref[:, pl.ds(pl.multiple_of(q * 2 * width, 2 * width), 2 * width)]
            both = jnp.dot(hidden, part, preferred_element_type=F32)
            low, high = both[:, :width], both[:, width:]
            one, two = jnp.where(core == 0, dx, dy), jnp.where(core == 0, dy, dx)
            keep_ref[one, two] = jnp.where(core == 0, low, high)
            send_ref[two, one] = jnp.where(core == 0, high, low)


def load_kernel(skipped, *refs):
    refs = refs[skipped:]
    sources, targets, sems = refs[:3], refs[3:6], refs[6]
    copies = [pltpu.make_async_copy(a, b, sems.at[i]) for i, (a, b) in enumerate(zip(sources, targets))]
    for copy in copies:
        copy.start()
    for copy in copies:
        copy.wait()


def loaded(after, weights):
    hbm = pl.BlockSpec(memory_space=pltpu.HBM)
    return pl.pallas_call(
        functools.partial(load_kernel, len(after)),
        out_shape=[jax.ShapeDtypeStruct(w.shape, w.dtype) for w in weights],
        in_specs=[hbm] * (len(after) + len(weights)),
        out_specs=[pl.BlockSpec(memory_space=pltpu.VMEM)] * len(weights),
        scratch_shapes=[pltpu.SemaphoreType.DMA((len(weights),))],
        compiler_params=pltpu.CompilerParams(vmem_limit_bytes=LOAD_MIB * MIB),
        cost_estimate=pl.CostEstimate(flops=1500000000, transcendentals=0, bytes_accessed=0),
    )(*after, *weights)


def stack_kernel(*refs):
    half = len(refs) - CHUNKS
    for chunk, out_ref in enumerate(refs[half:]):
        for k, ref in enumerate(refs[:half]):
            out_ref[k] = ref[chunk]


def stacked(pieces):
    out = jax.ShapeDtypeStruct((len(pieces),) + pieces[0].shape[1:], BF16)
    return pl.pallas_call(
        stack_kernel,
        out_shape=[out] * CHUNKS,
        compiler_params=pltpu.CompilerParams(vmem_limit_bytes=4 * MIB),
    )(*pieces)


def experts_of(where, own, partner, gains, gate, up, down):
    n = len(own)
    _, rows, width = own[0].shape
    model = gate.shape[1]
    vmem = pl.BlockSpec(memory_space=pltpu.VMEM)
    out = jax.ShapeDtypeStruct((n, n, rows, width), F32)
    return pl.pallas_call(
        functools.partial(expert_kernel, n),
        out_shape=(out, out),
        in_specs=[pl.BlockSpec(memory_space=pltpu.SMEM)] + [vmem] * (2 * n + 4),
        out_specs=(vmem, vmem),
        scratch_shapes=[pltpu.VMEM((rows, model), BF16)],
        compiler_params=pltpu.CompilerParams(vmem_limit_bytes=10 * MIB),
        cost_estimate=pl.CostEstimate(flops=3000000000, transcendentals=0, bytes_accessed=0),
    )(where, *own, *partner, gains, gate, up, down)


STEPS = 8
TOP = 32000.0
SPARE = 16


def scaled(blocks, refs):
    largest = functools.reduce(jnp.maximum, [jnp.abs(b) for group in blocks for b in group])
    largest = jnp.maximum(jnp.max(largest, axis=1, keepdims=True), 1e-32)
    code = jnp.ceil(STEPS * jnp.log2(largest)) + 1.0
    factor = TOP * jnp.exp2(code * (-1.0 / STEPS))
    rows, width = blocks[0][0].shape
    eye = lax.broadcasted_iota(jnp.int32, (width, width), 0) == lax.broadcasted_iota(jnp.int32, (width, width), 1)
    line = lax.broadcasted_iota(jnp.int32, (SPARE, width), 0)
    tile = jnp.zeros((SPARE, width), F32)
    for g in range(rows // width):
        part = jnp.sum(jnp.where(eye, code[g * width : (g + 1) * width], 0.0), axis=0, keepdims=True)
        tile = jnp.where(line == g, part, tile)
    for group, ref in zip(blocks, refs):
        for i, b in enumerate(group):
            ref[pl.ds(i * rows, rows), :] = jnp.round(b * factor).astype(jnp.int32).astype(jnp.int16)
        ref[pl.ds(len(group) * rows, SPARE), :] = tile.astype(jnp.int32).astype(jnp.int16)


def factors(ref, count, rows):
    tile = ref[pl.ds(count * rows, SPARE), :].astype(jnp.int32).astype(F32)
    width = tile.shape[1]
    code = jnp.concatenate([column(tile[g : g + 1, :]) for g in range(rows // width)], axis=0)
    return jnp.exp2(code * (1.0 / STEPS)) * (1.0 / TOP)


def widened(ref, i, rows):
    return ref[pl.ds(i * rows, rows), :].astype(jnp.int32).astype(F32)


def first_kernel(keep_ref, got_ref, own_ref, *out_refs):
    n = keep_ref.shape[0]
    for k2 in range(n):
        own_ref[k2] = keep_ref[0, k2] + got_ref[0, k2]
    blocks = [[keep_ref[k1, k2] + got_ref[k1, k2] for k2 in range(n)] for k1 in range(1, n)]
    scaled(blocks, out_refs)


def second_kernel(chunks, *refs):
    ins, sum_ref, out_refs = refs[: 4 * chunks], refs[4 * chunks], refs[4 * chunks + 1 :]
    n, rows, _ = ins[0].shape
    totals = []
    for chunk in range(chunks):
        own_ref, *got_refs = ins[4 * chunk : 4 * chunk + 4]
        by = [factors(got, n, rows) for got in got_refs]
        totals.append([])
        for k2 in range(n):
            total = own_ref[k2]
            for got, factor in zip(got_refs, by):
                total = total + widened(got, k2, rows) * factor
            totals[-1].append(total)
    totals = [jnp.concatenate(parts, axis=0) for parts in zip(*totals)]
    sum_ref[...] = totals[0]
    scaled([[total] for total in totals[1:]], out_refs)


def third_kernel(own_ref, *refs):
    got_refs, out_ref = refs[:-1], refs[-1]
    rows, _ = own_ref.shape
    total = own_ref[...]
    for got in got_refs:
        total = total + widened(got, 0, rows) * factors(got, 1, rows)
    out_ref[...] = total.astype(BF16)


def coded(blocks, rows, width):
    return jax.ShapeDtypeStruct((blocks * rows + SPARE, width), jnp.int16)


def started(keep, send):
    n, _, rows, width = keep.shape
    own, *parts = pl.pallas_call(
        first_kernel,
        out_shape=[jax.ShapeDtypeStruct((n, rows, width), F32)] + [coded(n, rows, width)] * (n - 1),
        compiler_params=pltpu.CompilerParams(vmem_limit_bytes=8 * MIB),
    )(keep, swapped(send))
    return [own] + [along(part, 0, k + 1) for k, part in enumerate(parts)]


def finished(chunks):
    n, rows, width = chunks[0][0].shape
    rows = rows * len(chunks)
    own, *parts = pl.pallas_call(
        functools.partial(second_kernel, len(chunks)),
        out_shape=[jax.ShapeDtypeStruct((rows, width), F32)] + [coded(1, rows, width)] * (n - 1),
        compiler_params=pltpu.CompilerParams(vmem_limit_bytes=4 * MIB),
    )(*[a for chunk in chunks for a in chunk])
    parts = [along(part, 1, k + 1) for k, part in enumerate(parts)]
    return pl.pallas_call(
        third_kernel,
        out_shape=jax.ShapeDtypeStruct((rows, width), BF16),
        compiler_params=pltpu.CompilerParams(vmem_limit_bytes=2 * MIB),
    )(own, *parts)


def local(tokens, norm_gain, route_logits, expert_ids, active, gate_weight, up_weight, down_weight):
    groups = lax.axis_size("expert")
    count, width = tokens.shape
    seat_limit = count // 2
    model = norm_gain.shape[0]
    where = jnp.stack([lax.axis_index(a) for a in TP]).astype(jnp.int32)
    gains = norm_gain.reshape(1, model)
    active_row, ids = active.reshape(1, count), expert_ids.T
    sent = pl.pallas_call(
        functools.partial(dispatch_kernel, seat_limit, groups),
        out_shape=jax.ShapeDtypeStruct((groups, seat_limit, width), BF16),
        compiler_params=pltpu.CompilerParams(vmem_limit_bytes=60 * MIB),
    )(ids, active_row, tokens)
    arriving = lax.all_to_all(sent, "expert", split_axis=0, concat_axis=0, tiled=True)
    n = lax.axis_size(TP[0])
    rows = arriving.reshape(CHUNKS, -1, width)
    first = [rows] + [along(rows, 0, k) for k in range(1, n)]
    weights = loaded((rows, gains, where), (gate_weight[0], up_weight[0], down_weight[0]))
    owns = []
    for stack in stacked(first):
        owns.append([stack] + [along(stack, 1, k) for k in range(1, n)])
    chunks = []
    for own in owns:
        partner = [swapped(a) for a in own]
        keep, send = experts_of(where, own, partner, gains, *weights)
        chunks.append(started(keep, send))
    returning = finished(chunks).reshape(groups, seat_limit, width)
    arrived = lax.all_to_all(returning, "expert", split_axis=0, concat_axis=0, tiled=True)
    return pl.pallas_call(
        functools.partial(combine_kernel, seat_limit, groups),
        out_shape=jax.ShapeDtypeStruct((count, width), BF16),
        compiler_params=pltpu.CompilerParams(vmem_limit_bytes=2 * MIB),
    )(ids, active_row, route_logits.T, arrived)


def solution(mesh):
    split = Mesh(
        mesh.devices.reshape(mesh.shape["expert"], 4, 4, 2), ("expert", "tp_0", "tp_1", "tp_2")
    )
    in_specs = (
        P("expert", TP),
        P(),
        P("expert", None),
        P("expert", None),
        P("expert"),
        P("expert", TP, None),
        P("expert", TP, None),
        P("expert", TP, None),
    )
    out_specs = P("expert", TP)
    return jax.shard_map(local, mesh=split, in_specs=in_specs, out_specs=out_specs, check_vma=False)
```

```python
import functools

import jax
import jax.numpy as jnp
from jax import lax
from jax.experimental import pallas as pl
from jax.experimental.pallas import tpu as pltpu
from jax.sharding import Mesh
from jax.sharding import PartitionSpec as P


TP = ("tp_0", "tp_1", "tp_2")
epsilon = 1e-05
F32, BF16 = jnp.float32, jnp.bfloat16
MIB = 1024 * 1024
STEP_ORDER = (2, 1, 3, 0)
LOAD_MIB = 41


def moved(array, target):
    nx, ny, cores = (lax.axis_size(a) for a in TP)
    flat = lambda x, y, core: ((x % nx) * ny + y % ny) * cores + core
    pairs = [
        (flat(x, y, core), flat(*target(x, y, core)))
        for x in range(nx)
        for y in range(ny)
        for core in range(cores)
    ]
    return lax.ppermute(array, TP, pairs)


def along(array, stage, step):
    def target(x, y, core):
        return (x + step, y, core) if core == stage else (x, y + step, core)

    return moved(array, target)


def swapped(array):
    return moved(array, lambda x, y, core: (x, y, 1 - core))


def column(row):
    count = row.shape[1]
    eye = lax.broadcasted_iota(jnp.int32, (count, count), 0) == lax.broadcasted_iota(jnp.int32, (count, count), 1)
    return jnp.sum(jnp.where(eye, row, jnp.zeros_like(row)), axis=1, keepdims=True)


def seats(ids_ref, active_ref, seat_limit, experts):
    count = ids_ref.shape[1]
    live = column(active_ref[...])
    first, second = column(ids_ref[0:1, :]), column(ids_ref[1:2, :])
    number = lax.broadcasted_iota(jnp.int32, (count, 128), 1)
    named = ((first == number) | (second == number)) & (live > 0)
    earlier = lax.broadcasted_iota(jnp.int32, (count, count), 1) < lax.broadcasted_iota(jnp.int32, (count, count), 0)
    place = jnp.dot(earlier.astype(BF16), named.astype(BF16), preferred_element_type=F32).astype(jnp.int32)
    place = jnp.where(named, place, -1)
    spot = lax.broadcasted_iota(jnp.int32, (count, seat_limit), 1)
    return live, first, second, [place[:, e : e + 1] == spot for e in range(experts)]


def dispatch_kernel(seat_limit, experts, ids_ref, active_ref, tokens_ref, out_ref):
    _, _, _, columns = seats(ids_ref, active_ref, seat_limit, experts)
    rows = tokens_ref[...]
    for e, hot in enumerate(columns):
        picked = lax.dot_general(
            hot.astype(BF16), rows, (((0,), (0,)), ((), ())), preferred_element_type=F32
        )
        out_ref[e] = picked.astype(BF16)


def combine_kernel(seat_limit, experts, ids_ref, active_ref, logits_ref, arrived_ref, out_ref):
    live, first, second, columns = seats(ids_ref, active_ref, seat_limit, experts)
    logits = logits_ref[...]
    raised = jnp.exp(logits - jnp.max(logits, axis=0, keepdims=True))
    probs = raised / jnp.sum(raised, axis=0, keepdims=True)
    total = jnp.zeros(out_ref.shape, F32)
    for k, ids in enumerate((first, second)):
        picked = jnp.zeros(out_ref.shape, F32)
        for e, hot in enumerate(columns):
            mine = (hot & (ids == e)).astype(BF16)
            picked = picked + jnp.dot(mine, arrived_ref[e], preferred_element_type=F32)
        total = total + column(probs[k : k + 1, :]) * live.astype(F32) * picked
    out_ref[...] = total.astype(BF16)


def hidden_kernel(n, where_ref, *refs):
    own, partner = refs[:n], refs[n : 2 * n]
    gain_ref, gate_ref, up_ref, hidden_ref, normed_ref = refs[2 * n :]
    x, y, core = where_ref[0], where_ref[1], where_ref[2]
    rows, _ = normed_ref.shape
    width = own[0].shape[-1]
    dims = (((1,), (1,)), ((), ()))
    for half in range(own[0].shape[1] // rows):
        span = slice(half * rows, (half + 1) * rows)
        squares = jnp.zeros((rows, width), F32)
        for pieces in (own, partner):
            for k2 in range(n):
                for k1 in range(n):
                    value = pieces[k2][k1, span].astype(F32)
                    squares = squares + value * value
        mean_square = jnp.sum(squares, axis=1, keepdims=True) / (2 * n * n * width)
        scale = lax.rsqrt(mean_square + epsilon)
        for pieces, parity in ((own, core), (partner, 1 - core)):
            for k2 in range(n):
                for k1 in range(n):
                    at = place(x - jnp.where(parity == 0, k1, k2), y - jnp.where(parity == 0, k2, k1), parity, n, width)
                    value = pieces[k2][k1, span].astype(F32) * scale * gain_ref[:, at].astype(F32)
                    normed_ref[:, at] = value.astype(BF16)
        normed = normed_ref[...]
        gate = lax.dot_general(normed, gate_ref[...], dims, preferred_element_type=F32)
        up = lax.dot_general(normed, up_ref[...], dims, preferred_element_type=F32)
        hidden_ref[span, :] = (gate / (1.0 + jnp.exp(-gate)) * up).astype(BF16)


def place(x, y, parity, n, width):
    t = (lax.rem(x + n, n) * n + lax.rem(y + n, n)) * 2 + parity
    return pl.ds(pl.multiple_of(t * width, width), width)


def down_kernel(n, step, where_ref, hidden_ref, down_ref, keep_ref, send_ref):
    x, y, core = where_ref[0], where_ref[1], where_ref[2]
    width = keep_ref.shape[-1]
    hidden = hidden_ref[...]
    for k2 in range(n):
        parts = [
            down_ref[:, place(x + jnp.where(p == 0, step, k2), y + jnp.where(p == 0, k2, step), p, n, width)]
            for p in (core, 1 - core)
        ]
        both = jnp.dot(hidden, jnp.concatenate(parts, axis=1), preferred_element_type=F32)
        keep_ref[k2], send_ref[k2] = both[:, :width], both[:, width:]


def load_kernel(skipped, *refs):
    refs = refs[skipped:]
    sources, targets, sems = refs[:3], refs[3:6], refs[6]
    copies = [pltpu.make_async_copy(a, b, sems.at[i]) for i, (a, b) in enumerate(zip(sources, targets))]
    for copy in copies:
        copy.start()
    for copy in copies:
        copy.wait()


def loaded(after, weights):
    hbm = pl.BlockSpec(memory_space=pltpu.HBM)
    return pl.pallas_call(
        functools.partial(load_kernel, len(after)),
        out_shape=[jax.ShapeDtypeStruct(w.shape, w.dtype) for w in weights],
        in_specs=[hbm] * (len(after) + len(weights)),
        out_specs=[pl.BlockSpec(memory_space=pltpu.VMEM)] * len(weights),
        scratch_shapes=[pltpu.SemaphoreType.DMA((len(weights),))],
        compiler_params=pltpu.CompilerParams(vmem_limit_bytes=LOAD_MIB * MIB),
        cost_estimate=pl.CostEstimate(flops=1500000000, transcendentals=0, bytes_accessed=0),
    )(*after, *weights)


VMEM = pl.BlockSpec(memory_space=pltpu.VMEM)
SMEM = pl.BlockSpec(memory_space=pltpu.SMEM)


def cost(flops):
    return pl.CostEstimate(flops=flops, transcendentals=0, bytes_accessed=0)


def stack_kernel(*refs):
    for k, ref in enumerate(refs[:-1]):
        refs[-1][k] = ref[...]


def stacked(pieces):
    return pl.pallas_call(
        stack_kernel,
        out_shape=jax.ShapeDtypeStruct((len(pieces),) + pieces[0].shape, BF16),
        compiler_params=pltpu.CompilerParams(vmem_limit_bytes=4 * MIB),
    )(*pieces)


def hidden_of(where, own, partner, gains, gate, up):
    n = len(own)
    rows = own[0].shape[1]
    units, model = gate.shape
    return pl.pallas_call(
        functools.partial(hidden_kernel, n),
        out_shape=jax.ShapeDtypeStruct((rows, units), BF16),
        in_specs=[SMEM] + [VMEM] * (2 * n + 3),
        out_specs=VMEM,
        scratch_shapes=[pltpu.VMEM((rows // 2, model), BF16)],
        compiler_params=pltpu.CompilerParams(vmem_limit_bytes=10 * MIB),
        cost_estimate=cost(4000000000),
    )(where, *own, *partner, gains, gate, up)


def down_of(step, where, hidden, down, n, width):
    out = jax.ShapeDtypeStruct((n, hidden.shape[0], width), F32)
    return pl.pallas_call(
        functools.partial(down_kernel, n, step),
        out_shape=(out, out),
        in_specs=[SMEM, VMEM, VMEM],
        out_specs=(VMEM, VMEM),
        compiler_params=pltpu.CompilerParams(vmem_limit_bytes=6 * MIB),
        cost_estimate=cost(500000000),
    )(where, hidden, down)


STEPS = 8
TOP = 32000.0
SPARE = 16


def scaled(blocks, refs):
    largest = functools.reduce(jnp.maximum, [jnp.abs(b) for group in blocks for b in group])
    largest = jnp.maximum(jnp.max(largest, axis=1, keepdims=True), 1e-32)
    code = jnp.ceil(STEPS * jnp.log2(largest)) + 1.0
    factor = TOP * jnp.exp2(code * (-1.0 / STEPS))
    rows, width = blocks[0][0].shape
    eye = lax.broadcasted_iota(jnp.int32, (width, width), 0) == lax.broadcasted_iota(jnp.int32, (width, width), 1)
    line = lax.broadcasted_iota(jnp.int32, (SPARE, width), 0)
    tile = jnp.zeros((SPARE, width), F32)
    for g in range(rows // width):
        part = jnp.sum(jnp.where(eye, code[g * width : (g + 1) * width], 0.0), axis=0, keepdims=True)
        tile = jnp.where(line == g, part, tile)
    for group, ref in zip(blocks, refs):
        for i, b in enumerate(group):
            ref[pl.ds(i * rows, rows), :] = jnp.round(b * factor).astype(jnp.int32).astype(jnp.int16)
        ref[pl.ds(len(group) * rows, SPARE), :] = tile.astype(jnp.int32).astype(jnp.int16)


def factors(ref, count, rows):
    tile = ref[pl.ds(count * rows, SPARE), :].astype(jnp.int32).astype(F32)
    width = tile.shape[1]
    code = jnp.concatenate([column(tile[g : g + 1, :]) for g in range(rows // width)], axis=0)
    return jnp.exp2(code * (1.0 / STEPS)) * (1.0 / TOP)


def widened(ref, i, rows):
    return ref[pl.ds(i * rows, rows), :].astype(jnp.int32).astype(F32)


def first_kernel(keep_ref, got_ref, out_ref):
    scaled([[keep_ref[k2] + got_ref[k2] for k2 in range(keep_ref.shape[0])]], [out_ref])


def second_kernel(n, keep_ref, got_ref, *refs):
    got_refs, sum_ref, out_refs = refs[: n - 1], refs[n - 1], refs[n:]
    rows = keep_ref.shape[1]
    by = [factors(got, n, rows) for got in got_refs]
    totals = []
    for k2 in range(n):
        total = keep_ref[k2] + got_ref[k2]
        for got, factor in zip(got_refs, by):
            total = total + widened(got, k2, rows) * factor
        totals.append(total)
    sum_ref[...] = totals[0]
    scaled([[total] for total in totals[1:]], out_refs)


def third_kernel(own_ref, *refs):
    got_refs, out_ref = refs[:-1], refs[-1]
    rows, _ = own_ref.shape
    total = own_ref[...]
    for got in got_refs:
        total = total + widened(got, 0, rows) * factors(got, 1, rows)
    out_ref[...] = total.astype(BF16)


def coded(blocks, rows, width):
    return jax.ShapeDtypeStruct((blocks * rows + SPARE, width), jnp.int16)


def first_sum(keep, got):
    return pl.pallas_call(
        first_kernel,
        out_shape=coded(*keep.shape),
        compiler_params=pltpu.CompilerParams(vmem_limit_bytes=6 * MIB),
        cost_estimate=cost(100000000),
    )(keep, got)


def finished(keep, got, parts):
    n, rows, width = keep.shape
    own, *parts = pl.pallas_call(
        functools.partial(second_kernel, n),
        out_shape=[jax.ShapeDtypeStruct((rows, width), F32)] + [coded(1, rows, width)] * (n - 1),
        compiler_params=pltpu.CompilerParams(vmem_limit_bytes=4 * MIB),
    )(keep, got, *parts)
    parts = [along(part, 1, k + 1) for k, part in enumerate(parts)]
    return pl.pallas_call(
        third_kernel,
        out_shape=jax.ShapeDtypeStruct((rows, width), BF16),
        compiler_params=pltpu.CompilerParams(vmem_limit_bytes=2 * MIB),
    )(own, *parts)


def local(tokens, norm_gain, route_logits, expert_ids, active, gate_weight, up_weight, down_weight):
    groups = lax.axis_size("expert")
    count, width = tokens.shape
    seat_limit = count // 2
    n = lax.axis_size(TP[0])
    model = norm_gain.shape[0]
    where = jnp.stack([lax.axis_index(a) for a in TP]).astype(jnp.int32)
    gains = norm_gain.reshape(1, model)
    active_row, ids = active.reshape(1, count), expert_ids.T
    sent = pl.pallas_call(
        functools.partial(dispatch_kernel, seat_limit, groups),
        out_shape=jax.ShapeDtypeStruct((groups, seat_limit, width), BF16),
        compiler_params=pltpu.CompilerParams(vmem_limit_bytes=60 * MIB),
    )(ids, active_row, tokens)
    arriving = lax.all_to_all(sent, "expert", split_axis=0, concat_axis=0, tiled=True)
    n = lax.axis_size(TP[0])
    rows = arriving.reshape(-1, width)
    stack = stacked([rows] + [along(rows, 0, k) for k in range(1, n)])
    own = [stack] + [along(stack, 1, k) for k in range(1, n)]
    gate, up, down = loaded((rows, gains, where), (gate_weight[0], up_weight[0], down_weight[0]))
    partner = [swapped(a) for a in own]
    hidden = hidden_of(where, own, partner, gains, gate, up)
    keeps, gots = {}, {}
    for step in STEP_ORDER:
        keeps[step], send = down_of(step, where, hidden, down, n, width)
        gots[step] = swapped(send)
    parts = []
    for step in range(1, n):
        part = first_sum(keeps[step], gots[step])
        parts.append(along(part, 0, step))
    returning = finished(keeps[0], gots[0], parts).reshape(groups, seat_limit, width)
    arrived = lax.all_to_all(returning, "expert", split_axis=0, concat_axis=0, tiled=True)
    return pl.pallas_call(
        functools.partial(combine_kernel, seat_limit, groups),
        out_shape=jax.ShapeDtypeStruct((count, width), BF16),
        compiler_params=pltpu.CompilerParams(vmem_limit_bytes=2 * MIB),
    )(ids, active_row, route_logits.T, arrived)


def solution(mesh):
    split = Mesh(
        mesh.devices.reshape(mesh.shape["expert"], 4, 4, 2), ("expert", "tp_0", "tp_1", "tp_2")
    )
    in_specs = (
        P("expert", TP),
        P(),
        P("expert", None),
        P("expert", None),
        P("expert"),
        P("expert", TP, None),
        P("expert", TP, None),
        P("expert", TP, None),
    )
    out_specs = P("expert", TP)
    return jax.shard_map(local, mesh=split, in_specs=in_specs, out_specs=out_specs, check_vma=False)
```

```python
import functools

import jax
import jax.numpy as jnp
from jax import lax
from jax.experimental import pallas as pl
from jax.experimental.pallas import tpu as pltpu
from jax.sharding import Mesh
from jax.sharding import PartitionSpec as P


TP = ("tp_0", "tp_1", "tp_2")
epsilon = 1e-05
F32, BF16 = jnp.float32, jnp.bfloat16
MIB = 1024 * 1024
LOAD_MIB = 41


def moved(array, target):
    nx, ny, cores = (lax.axis_size(a) for a in TP)
    flat = lambda x, y, core: ((x % nx) * ny + y % ny) * cores + core
    pairs = [
        (flat(x, y, core), flat(*target(x, y, core)))
        for x in range(nx)
        for y in range(ny)
        for core in range(cores)
    ]
    return lax.ppermute(array, TP, pairs)


def along(array, stage, step):
    def target(x, y, core):
        return (x + step, y, core) if core == stage else (x, y + step, core)

    return moved(array, target)


def swapped(array):
    return moved(array, lambda x, y, core: (x, y, 1 - core))


def column(row):
    count = row.shape[1]
    eye = lax.broadcasted_iota(jnp.int32, (count, count), 0) == lax.broadcasted_iota(jnp.int32, (count, count), 1)
    return jnp.sum(jnp.where(eye, row, jnp.zeros_like(row)), axis=1, keepdims=True)


def seats(ids_ref, active_ref, seat_limit, experts):
    count = ids_ref.shape[1]
    live = column(active_ref[...])
    first, second = column(ids_ref[0:1, :]), column(ids_ref[1:2, :])
    number = lax.broadcasted_iota(jnp.int32, (count, 128), 1)
    named = ((first == number) | (second == number)) & (live > 0)
    earlier = lax.broadcasted_iota(jnp.int32, (count, count), 1) < lax.broadcasted_iota(jnp.int32, (count, count), 0)
    place = jnp.dot(earlier.astype(BF16), named.astype(BF16), preferred_element_type=F32).astype(jnp.int32)
    place = jnp.where(named, place, -1)
    spot = lax.broadcasted_iota(jnp.int32, (count, seat_limit), 1)
    return live, first, second, [place[:, e : e + 1] == spot for e in range(experts)]


def dispatch_kernel(seat_limit, experts, ids_ref, active_ref, tokens_ref, out_ref):
    _, _, _, columns = seats(ids_ref, active_ref, seat_limit, experts)
    rows = tokens_ref[...]
    for e, hot in enumerate(columns):
        picked = lax.dot_general(
            hot.astype(BF16), rows, (((0,), (0,)), ((), ())), preferred_element_type=F32
        )
        out_ref[e] = picked.astype(BF16)


def combine_kernel(seat_limit, experts, ids_ref, active_ref, logits_ref, arrived_ref, out_ref):
    live, first, second, columns = seats(ids_ref, active_ref, seat_limit, experts)
    logits = logits_ref[...]
    raised = jnp.exp(logits - jnp.max(logits, axis=0, keepdims=True))
    probs = raised / jnp.sum(raised, axis=0, keepdims=True)
    total = jnp.zeros(out_ref.shape, F32)
    for k, ids in enumerate((first, second)):
        picked = jnp.zeros(out_ref.shape, F32)
        for e, hot in enumerate(columns):
            mine = (hot & (ids == e)).astype(BF16)
            picked = picked + jnp.dot(mine, arrived_ref[e], preferred_element_type=F32)
        total = total + column(probs[k : k + 1, :]) * live.astype(F32) * picked
    out_ref[...] = total.astype(BF16)


def hidden_kernel(n, where_ref, *refs):
    own, partner = refs[: 2 * n], refs[2 * n : 4 * n]
    gain_ref, gate_ref, up_ref, hidden_ref, normed_ref = refs[4 * n :]
    x, y, core = where_ref[0], where_ref[1], where_ref[2]
    rows, _ = normed_ref.shape
    width = own[0].shape[-1]
    steps = [(k1, k2) for k2 in range(n) for k1 in range(n)]
    dims = (((1,), (1,)), ((), ()))

    def piece(pieces, k1, k2):
        return pieces[2 * k2 + k1 // (n // 2)][k1 % (n // 2), span].astype(F32)

    for half in range(own[0].shape[1] // rows):
        span = slice(half * rows, (half + 1) * rows)
        squares = jnp.zeros((rows, width), F32)
        for pieces in (own, partner):
            for k1, k2 in steps:
                value = piece(pieces, k1, k2)
                squares = squares + value * value
        mean_square = jnp.sum(squares, axis=1, keepdims=True) / (2 * n * n * width)
        scale = lax.rsqrt(mean_square + epsilon)
        for pieces, parity in ((own, core), (partner, 1 - core)):
            for k1, k2 in steps:
                at = place(x - jnp.where(parity == 0, k1, k2), y - jnp.where(parity == 0, k2, k1), parity, n, width)
                value = piece(pieces, k1, k2) * scale * gain_ref[:, at].astype(F32)
                normed_ref[:, at] = value.astype(BF16)
        normed = normed_ref[...]
        gate = lax.dot_general(normed, gate_ref[...], dims, preferred_element_type=F32)
        up = lax.dot_general(normed, up_ref[...], dims, preferred_element_type=F32)
        hidden_ref[span, :] = (gate / (1.0 + jnp.exp(-gate)) * up).astype(BF16)


def place(x, y, parity, n, width):
    t = (lax.rem(x + n, n) * n + lax.rem(y + n, n)) * 2 + parity
    return pl.ds(pl.multiple_of(t * width, width), width)


def down_kernel(n, step, where_ref, hidden_ref, down_ref, keep_ref, send_ref):
    x, y, core = where_ref[0], where_ref[1], where_ref[2]
    width = keep_ref.shape[-1]
    hidden = hidden_ref[...]
    for k2 in range(n):
        parts = [
            down_ref[:, place(x + jnp.where(p == 0, step, k2), y + jnp.where(p == 0, k2, step), p, n, width)]
            for p in (core, 1 - core)
        ]
        both = jnp.dot(hidden, jnp.concatenate(parts, axis=1), preferred_element_type=F32)
        keep_ref[k2], send_ref[k2] = both[:, :width], both[:, width:]


def load_kernel(skipped, *refs):
    refs = refs[skipped:]
    sources, targets, sems = refs[:3], refs[3:6], refs[6]
    copies = [pltpu.make_async_copy(a, b, sems.at[i]) for i, (a, b) in enumerate(zip(sources, targets))]
    for copy in copies:
        copy.start()
    for copy in copies:
        copy.wait()


def loaded(after, weights):
    hbm = pl.BlockSpec(memory_space=pltpu.HBM)
    return pl.pallas_call(
        functools.partial(load_kernel, len(after)),
        out_shape=[jax.ShapeDtypeStruct(w.shape, w.dtype) for w in weights],
        in_specs=[hbm] * (len(after) + len(weights)),
        out_specs=[pl.BlockSpec(memory_space=pltpu.VMEM)] * len(weights),
        scratch_shapes=[pltpu.SemaphoreType.DMA((len(weights),))],
        compiler_params=pltpu.CompilerParams(vmem_limit_bytes=LOAD_MIB * MIB),
        cost_estimate=pl.CostEstimate(flops=1500000000, transcendentals=0, bytes_accessed=0),
    )(*after, *weights)


VMEM = pl.BlockSpec(memory_space=pltpu.VMEM)
SMEM = pl.BlockSpec(memory_space=pltpu.SMEM)


def cost(flops):
    return pl.CostEstimate(flops=flops, transcendentals=0, bytes_accessed=0)


def stack_kernel(*refs):
    half = (len(refs) - 2) // 2
    for k, ref in enumerate(refs[:-2]):
        refs[-2 + k // half][k % half] = ref[...]


def stacked(pieces):
    out = jax.ShapeDtypeStruct((len(pieces) // 2,) + pieces[0].shape, BF16)
    return pl.pallas_call(
        stack_kernel,
        out_shape=(out, out),
        compiler_params=pltpu.CompilerParams(vmem_limit_bytes=4 * MIB),
    )(*pieces)


def hidden_of(where, own, partner, gains, gate, up):
    n = len(own) // 2
    rows = own[0].shape[1]
    units, model = gate.shape
    return pl.pallas_call(
        functools.partial(hidden_kernel, n),
        out_shape=jax.ShapeDtypeStruct((rows, units), BF16),
        in_specs=[SMEM] + [VMEM] * (4 * n + 3),
        out_specs=VMEM,
        scratch_shapes=[pltpu.VMEM((rows // 2, model), BF16)],
        compiler_params=pltpu.CompilerParams(vmem_limit_bytes=10 * MIB),
        cost_estimate=cost(4000000000),
    )(where, *own, *partner, gains, gate, up)


def down_of(step, where, hidden, down, n, width):
    out = jax.ShapeDtypeStruct((n, hidden.shape[0], width), F32)
    return pl.pallas_call(
        functools.partial(down_kernel, n, step),
        out_shape=(out, out),
        in_specs=[SMEM, VMEM, VMEM],
        out_specs=(VMEM, VMEM),
        compiler_params=pltpu.CompilerParams(vmem_limit_bytes=6 * MIB),
        cost_estimate=cost(500000000),
    )(where, hidden, down)


STEPS = 8
TOP = 32000.0
SPARE = 16


def scaled(blocks, refs):
    largest = functools.reduce(jnp.maximum, [jnp.abs(b) for group in blocks for b in group])
    largest = jnp.maximum(jnp.max(largest, axis=1, keepdims=True), 1e-32)
    code = jnp.ceil(STEPS * jnp.log2(largest)) + 1.0
    factor = TOP * jnp.exp2(code * (-1.0 / STEPS))
    rows, width = blocks[0][0].shape
    eye = lax.broadcasted_iota(jnp.int32, (width, width), 0) == lax.broadcasted_iota(jnp.int32, (width, width), 1)
    line = lax.broadcasted_iota(jnp.int32, (SPARE, width), 0)
    tile = jnp.zeros((SPARE, width), F32)
    for g in range(rows // width):
        part = jnp.sum(jnp.where(eye, code[g * width : (g + 1) * width], 0.0), axis=0, keepdims=True)
        tile = jnp.where(line == g, part, tile)
    for group, ref in zip(blocks, refs):
        for i, b in enumerate(group):
            ref[pl.ds(i * rows, rows), :] = jnp.round(b * factor).astype(jnp.int32).astype(jnp.int16)
        ref[pl.ds(len(group) * rows, SPARE), :] = tile.astype(jnp.int32).astype(jnp.int16)


def factors(ref, count, rows):
    tile = ref[pl.ds(count * rows, SPARE), :].astype(jnp.int32).astype(F32)
    width = tile.shape[1]
    code = jnp.concatenate([column(tile[g : g + 1, :]) for g in range(rows // width)], axis=0)
    return jnp.exp2(code * (1.0 / STEPS)) * (1.0 / TOP)


def widened(ref, i, rows):
    return ref[pl.ds(i * rows, rows), :].astype(jnp.int32).astype(F32)


def first_kernel(halves, keep_ref, got_ref, *out_refs):
    half = keep_ref.shape[0] // 2
    scaled([[keep_ref[half * h + i] + got_ref[half * h + i] for i in range(half)] for h in halves], out_refs)


def relay_kernel(h, keep_ref, got_ref, passed_ref, out_ref):
    half, rows = keep_ref.shape[0] // 2, keep_ref.shape[1]
    factor = factors(passed_ref, half, rows)
    blocks = [
        keep_ref[half * h + i] + got_ref[half * h + i] + widened(passed_ref, i, rows) * factor
        for i in range(half)
    ]
    scaled([blocks], [out_ref])


def second_kernel(n, keep_ref, got_ref, *refs):
    got_refs, sum_ref, out_refs = refs[:4], refs[4], refs[5:]
    half, rows = n // 2, keep_ref.shape[1]
    by = [factors(got, half, rows) for got in got_refs]
    totals = []
    for k2 in range(n):
        total = keep_ref[k2] + got_ref[k2]
        for side in range(2):
            i = 2 * side + k2 // half
            total = total + widened(got_refs[i], k2 % half, rows) * by[i]
        totals.append(total)
    sum_ref[...] = totals[0]
    scaled([[total] for total in totals[1:]], out_refs)


def third_kernel(own_ref, *refs):
    got_refs, out_ref = refs[:-1], refs[-1]
    rows, _ = own_ref.shape
    total = own_ref[...]
    for got in got_refs:
        total = total + widened(got, 0, rows) * factors(got, 1, rows)
    out_ref[...] = total.astype(BF16)


def coded(blocks, rows, width):
    return jax.ShapeDtypeStruct((blocks * rows + SPARE, width), jnp.int16)


def first_sum(halves, keep, got):
    n, rows, width = keep.shape
    return pl.pallas_call(
        functools.partial(first_kernel, halves),
        out_shape=[coded(n // 2, rows, width)] * len(halves),
        compiler_params=pltpu.CompilerParams(vmem_limit_bytes=6 * MIB),
        cost_estimate=cost(100000000),
    )(keep, got)


def relayed(half, keep, got, passed):
    n, rows, width = keep.shape
    return pl.pallas_call(
        functools.partial(relay_kernel, half),
        out_shape=coded(n // 2, rows, width),
        compiler_params=pltpu.CompilerParams(vmem_limit_bytes=6 * MIB),
        cost_estimate=cost(100000000),
    )(keep, got, passed)


def finished(keep, got, parts):
    n, rows, width = keep.shape
    own, *parts = pl.pallas_call(
        functools.partial(second_kernel, n),
        out_shape=[jax.ShapeDtypeStruct((rows, width), F32)] + [coded(1, rows, width)] * (n - 1),
        compiler_params=pltpu.CompilerParams(vmem_limit_bytes=4 * MIB),
    )(keep, got, *parts)
    parts = [along(part, 1, k + 1) for k, part in enumerate(parts)]
    return pl.pallas_call(
        third_kernel,
        out_shape=jax.ShapeDtypeStruct((rows, width), BF16),
        compiler_params=pltpu.CompilerParams(vmem_limit_bytes=2 * MIB),
    )(own, *parts)


def local(tokens, norm_gain, route_logits, expert_ids, active, gate_weight, up_weight, down_weight):
    groups = lax.axis_size("expert")
    count, width = tokens.shape
    seat_limit = count // 2
    n = lax.axis_size(TP[0])
    model = norm_gain.shape[0]
    where = jnp.stack([lax.axis_index(a) for a in TP]).astype(jnp.int32)
    gains = norm_gain.reshape(1, model)
    active_row, ids = active.reshape(1, count), expert_ids.T
    sent = pl.pallas_call(
        functools.partial(dispatch_kernel, seat_limit, groups),
        out_shape=jax.ShapeDtypeStruct((groups, seat_limit, width), BF16),
        compiler_params=pltpu.CompilerParams(vmem_limit_bytes=60 * MIB),
    )(ids, active_row, tokens)
    arriving = lax.all_to_all(sent, "expert", split_axis=0, concat_axis=0, tiled=True)
    n = lax.axis_size(TP[0])
    rows = arriving.reshape(-1, width)
    spread = [along(rows, 0, k) for k in range(1, n)]
    gate, up, down = loaded((rows, gains, where), (gate_weight[0], up_weight[0], down_weight[0]))
    low, high = stacked([rows] + spread)
    low_1, high_3 = along(low, 1, 1), along(high, 1, -1)
    high_1, low_3 = along(high, 1, 1), along(low, 1, -1)
    low_2, high_2 = along(low_1, 1, 1), along(high_3, 1, -1)
    own = [low, high, low_1, high_1, low_2, high_2, low_3, high_3]
    partner = [swapped(a) for a in own]
    hidden = hidden_of(where, own, partner, gains, gate, up)
    keeps, gots = {}, {}
    for step in (2, 1, 3, 0):
        keeps[step], send = down_of(step, where, hidden, down, n, width)
        gots[step] = swapped(send)
    low, high = first_sum((0, 1), keeps[2], gots[2])
    low, high = along(low, 0, 1), along(high, 0, -1)
    (high_1,), (low_3,) = first_sum((1,), keeps[1], gots[1]), first_sum((0,), keeps[3], gots[3])
    high_1, low_3 = along(high_1, 0, 1), along(low_3, 0, -1)
    low_1, high_3 = relayed(0, keeps[1], gots[1], low), relayed(1, keeps[3], gots[3], high)
    low_1, high_3 = along(low_1, 0, 1), along(high_3, 0, -1)
    returning = finished(keeps[0], gots[0], [low_1, high_1, low_3, high_3])
    returning = returning.reshape(groups, seat_limit, width)
    arrived = lax.all_to_all(returning, "expert", split_axis=0, concat_axis=0, tiled=True)
    return pl.pallas_call(
        functools.partial(combine_kernel, seat_limit, groups),
        out_shape=jax.ShapeDtypeStruct((count, width), BF16),
        compiler_params=pltpu.CompilerParams(vmem_limit_bytes=2 * MIB),
    )(ids, active_row, route_logits.T, arrived)


def solution(mesh):
    split = Mesh(
        mesh.devices.reshape(mesh.shape["expert"], 4, 4, 2), ("expert", "tp_0", "tp_1", "tp_2")
    )
    in_specs = (
        P("expert", TP),
        P(),
        P("expert", None),
        P("expert", None),
        P("expert"),
        P("expert", TP, None),
        P("expert", TP, None),
        P("expert", TP, None),
    )
    out_specs = P("expert", TP)
    return jax.shard_map(local, mesh=split, in_specs=in_specs, out_specs=out_specs, check_vma=False)
```

```python
import functools

import jax
import jax.numpy as jnp
from jax import lax
from jax.experimental import pallas as pl
from jax.experimental.pallas import tpu as pltpu
from jax.sharding import Mesh
from jax.sharding import PartitionSpec as P


TP = ("tp_0", "tp_1", "tp_2")
epsilon = 1e-05
F32, BF16 = jnp.float32, jnp.bfloat16
MIB = 1024 * 1024
CHUNKS = 2
STACK_FLOPS = 5000000000


def moved(array, target):
    nx, ny, cores = (lax.axis_size(a) for a in TP)
    flat = lambda x, y, core: ((x % nx) * ny + y % ny) * cores + core
    pairs = [
        (flat(x, y, core), flat(*target(x, y, core)))
        for x in range(nx)
        for y in range(ny)
        for core in range(cores)
    ]
    return lax.ppermute(array, TP, pairs)


def along(array, stage, step):
    def target(x, y, core):
        return (x + step, y, core) if core == stage else (x, y + step, core)

    return moved(array, target)


def swapped(array):
    return moved(array, lambda x, y, core: (x, y, 1 - core))


def column(row):
    count = row.shape[1]
    eye = lax.broadcasted_iota(jnp.int32, (count, count), 0) == lax.broadcasted_iota(jnp.int32, (count, count), 1)
    return jnp.sum(jnp.where(eye, row, jnp.zeros_like(row)), axis=1, keepdims=True)


def seats(ids_ref, active_ref, seat_limit, experts):
    count = ids_ref.shape[1]
    live = column(active_ref[...])
    first, second = column(ids_ref[0:1, :]), column(ids_ref[1:2, :])
    number = lax.broadcasted_iota(jnp.int32, (count, 128), 1)
    named = ((first == number) | (second == number)) & (live > 0)
    earlier = lax.broadcasted_iota(jnp.int32, (count, count), 1) < lax.broadcasted_iota(jnp.int32, (count, count), 0)
    place = jnp.dot(earlier.astype(BF16), named.astype(BF16), preferred_element_type=F32).astype(jnp.int32)
    place = jnp.where(named, place, -1)
    spot = lax.broadcasted_iota(jnp.int32, (count, seat_limit), 1)
    return live, first, second, [place[:, e : e + 1] == spot for e in range(experts)]


def dispatch_kernel(seat_limit, experts, ids_ref, active_ref, tokens_ref, out_ref):
    _, _, _, columns = seats(ids_ref, active_ref, seat_limit, experts)
    rows = tokens_ref[...]
    for e, hot in enumerate(columns):
        picked = lax.dot_general(
            hot.astype(BF16), rows, (((0,), (0,)), ((), ())), preferred_element_type=F32
        )
        out_ref[e] = picked.astype(BF16)


def combine_kernel(seat_limit, experts, ids_ref, active_ref, logits_ref, arrived_ref, out_ref):
    live, first, second, columns = seats(ids_ref, active_ref, seat_limit, experts)
    logits = logits_ref[...]
    raised = jnp.exp(logits - jnp.max(logits, axis=0, keepdims=True))
    probs = raised / jnp.sum(raised, axis=0, keepdims=True)
    total = jnp.zeros(out_ref.shape, F32)
    for k, ids in enumerate((first, second)):
        picked = jnp.zeros(out_ref.shape, F32)
        for e, hot in enumerate(columns):
            mine = (hot & (ids == e)).astype(BF16)
            picked = picked + jnp.dot(mine, arrived_ref[e], preferred_element_type=F32)
        total = total + column(probs[k : k + 1, :]) * live.astype(F32) * picked
    out_ref[...] = total.astype(BF16)


def expert_kernel(n, where_ref, *refs):
    own, partner = refs[:n], refs[n : 2 * n]
    gain_ref, gate_ref, up_ref, down_ref, keep_ref, send_ref, normed_ref = refs[2 * n :]
    x, y, core = where_ref[0], where_ref[1], where_ref[2]
    rows = normed_ref.shape[0]
    width = own[0].shape[-1]
    squares = jnp.zeros((rows, width), F32)
    for pieces in (own, partner):
        for k2 in range(n):
            for k1 in range(n):
                value = pieces[k2][k1].astype(F32)
                squares = squares + value * value
    mean_square = jnp.sum(squares, axis=1, keepdims=True) / (2 * n * n * width)
    scale = lax.rsqrt(mean_square + epsilon)
    for pieces, parity in ((own, core), (partner, 1 - core)):
        for k2 in range(n):
            for k1 in range(n):
                at_x = lax.rem(x - jnp.where(parity == 0, k1, k2) + n, n)
                at_y = lax.rem(y - jnp.where(parity == 0, k2, k1) + n, n)
                t = (at_x * n + at_y) * 2 + parity
                value = pieces[k2][k1].astype(F32) * scale * gain_ref[:, pl.ds(pl.multiple_of(t * width, width), width)].astype(F32)
                normed_ref[:, pl.ds(pl.multiple_of(t * width, width), width)] = value.astype(BF16)
    normed = normed_ref[...]
    dims = (((1,), (1,)), ((), ()))
    gate = lax.dot_general(normed, gate_ref[...], dims, preferred_element_type=F32)
    up = lax.dot_general(normed, up_ref[...], dims, preferred_element_type=F32)
    hidden = (gate / (1.0 + jnp.exp(-gate)) * up).astype(BF16)
    for dx in range(n):
        for dy in range(n):
            q = lax.rem(x + dx, n) * n + lax.rem(y + dy, n)
            part = down_ref[:, pl.ds(pl.multiple_of(q * 2 * width, 2 * width), 2 * width)]
            both = jnp.dot(hidden, part, preferred_element_type=F32)
            low, high = both[:, :width], both[:, width:]
            one, two = jnp.where(core == 0, dx, dy), jnp.where(core == 0, dy, dx)
            keep_ref[one, two] = jnp.where(core == 0, low, high)
            send_ref[two, one] = jnp.where(core == 0, high, low)


def stack_kernel(skipped, *refs):
    refs = refs[skipped:]
    half = len(refs) - CHUNKS
    for chunk, out_ref in enumerate(refs[half:]):
        for k, ref in enumerate(refs[:half]):
            out_ref[k] = ref[chunk]


def stacked(after, pieces):
    out = jax.ShapeDtypeStruct((len(pieces),) + pieces[0].shape[1:], BF16)
    return pl.pallas_call(
        functools.partial(stack_kernel, len(after)),
        out_shape=[out] * CHUNKS,
        in_specs=[pl.BlockSpec(memory_space=pltpu.HBM)] * len(after)
        + [pl.BlockSpec(memory_space=pltpu.VMEM)] * len(pieces),
        out_specs=[pl.BlockSpec(memory_space=pltpu.VMEM)] * CHUNKS,
        compiler_params=pltpu.CompilerParams(vmem_limit_bytes=4 * MIB),
        cost_estimate=pl.CostEstimate(flops=STACK_FLOPS, transcendentals=0, bytes_accessed=0),
    )(*after, *pieces)


def experts_of(where, own, partner, gains, gate, up, down):
    n = len(own)
    _, rows, width = own[0].shape
    model = gate.shape[1]
    vmem = pl.BlockSpec(memory_space=pltpu.VMEM)
    out = jax.ShapeDtypeStruct((n, n, rows, width), F32)
    return pl.pallas_call(
        functools.partial(expert_kernel, n),
        out_shape=(out, out),
        in_specs=[pl.BlockSpec(memory_space=pltpu.SMEM)] + [vmem] * (2 * n + 4),
        out_specs=(vmem, vmem),
        scratch_shapes=[pltpu.VMEM((rows, model), BF16)],
        compiler_params=pltpu.CompilerParams(vmem_limit_bytes=10 * MIB),
        cost_estimate=pl.CostEstimate(flops=3000000000, transcendentals=0, bytes_accessed=0),
    )(where, *own, *partner, gains, gate, up, down)


STEPS = 8
TOP = 32000.0
SPARE = 16


def scaled(blocks, refs):
    largest = functools.reduce(jnp.maximum, [jnp.abs(b) for group in blocks for b in group])
    largest = jnp.maximum(jnp.max(largest, axis=1, keepdims=True), 1e-32)
    code = jnp.ceil(STEPS * jnp.log2(largest)) + 1.0
    factor = TOP * jnp.exp2(code * (-1.0 / STEPS))
    rows, width = blocks[0][0].shape
    eye = lax.broadcasted_iota(jnp.int32, (width, width), 0) == lax.broadcasted_iota(jnp.int32, (width, width), 1)
    line = lax.broadcasted_iota(jnp.int32, (SPARE, width), 0)
    tile = jnp.zeros((SPARE, width), F32)
    for g in range(rows // width):
        part = jnp.sum(jnp.where(eye, code[g * width : (g + 1) * width], 0.0), axis=0, keepdims=True)
        tile = jnp.where(line == g, part, tile)
    for group, ref in zip(blocks, refs):
        for i, b in enumerate(group):
            ref[pl.ds(i * rows, rows), :] = jnp.round(b * factor).astype(jnp.int32).astype(jnp.int16)
        ref[pl.ds(len(group) * rows, SPARE), :] = tile.astype(jnp.int32).astype(jnp.int16)


def factors(ref, count, rows):
    tile = ref[pl.ds(count * rows, SPARE), :].astype(jnp.int32).astype(F32)
    width = tile.shape[1]
    code = jnp.concatenate([column(tile[g : g + 1, :]) for g in range(rows // width)], axis=0)
    return jnp.exp2(code * (1.0 / STEPS)) * (1.0 / TOP)


def widened(ref, i, rows):
    return ref[pl.ds(i * rows, rows), :].astype(jnp.int32).astype(F32)


def first_kernel(keep_ref, got_ref, own_ref, *out_refs):
    n = keep_ref.shape[0]
    for k2 in range(n):
        own_ref[k2] = keep_ref[0, k2] + got_ref[0, k2]
    blocks = [[keep_ref[k1, k2] + got_ref[k1, k2] for k2 in range(n)] for k1 in range(1, n)]
    scaled(blocks, out_refs)


def second_kernel(chunks, *refs):
    ins, sum_ref, out_refs = refs[: 4 * chunks], refs[4 * chunks], refs[4 * chunks + 1 :]
    n, rows, _ = ins[0].shape
    totals = []
    for chunk in range(chunks):
        own_ref, *got_refs = ins[4 * chunk : 4 * chunk + 4]
        by = [factors(got, n, rows) for got in got_refs]
        totals.append([])
        for k2 in range(n):
            total = own_ref[k2]
            for got, factor in zip(got_refs, by):
                total = total + widened(got, k2, rows) * factor
            totals[-1].append(total)
    totals = [jnp.concatenate(parts, axis=0) for parts in zip(*totals)]
    sum_ref[...] = totals[0]
    scaled([[total] for total in totals[1:]], out_refs)


def third_kernel(own_ref, *refs):
    got_refs, out_ref = refs[:-1], refs[-1]
    rows, _ = own_ref.shape
    total = own_ref[...]
    for got in got_refs:
        total = total + widened(got, 0, rows) * factors(got, 1, rows)
    out_ref[...] = total.astype(BF16)


def coded(blocks, rows, width):
    return jax.ShapeDtypeStruct((blocks * rows + SPARE, width), jnp.int16)


def started(keep, send):
    n, _, rows, width = keep.shape
    own, *parts = pl.pallas_call(
        first_kernel,
        out_shape=[jax.ShapeDtypeStruct((n, rows, width), F32)] + [coded(n, rows, width)] * (n - 1),
        compiler_params=pltpu.CompilerParams(vmem_limit_bytes=8 * MIB),
    )(keep, swapped(send))
    return [own] + [along(part, 0, k + 1) for k, part in enumerate(parts)]


def finished(chunks):
    n, rows, width = chunks[0][0].shape
    rows = rows * len(chunks)
    own, *parts = pl.pallas_call(
        functools.partial(second_kernel, len(chunks)),
        out_shape=[jax.ShapeDtypeStruct((rows, width), F32)] + [coded(1, rows, width)] * (n - 1),
        compiler_params=pltpu.CompilerParams(vmem_limit_bytes=4 * MIB),
    )(*[a for chunk in chunks for a in chunk])
    parts = [along(part, 1, k + 1) for k, part in enumerate(parts)]
    return pl.pallas_call(
        third_kernel,
        out_shape=jax.ShapeDtypeStruct((rows, width), BF16),
        compiler_params=pltpu.CompilerParams(vmem_limit_bytes=2 * MIB),
    )(own, *parts)


def local(tokens, norm_gain, route_logits, expert_ids, active, gate_weight, up_weight, down_weight):
    groups = lax.axis_size("expert")
    count, width = tokens.shape
    seat_limit = count // 2
    model = norm_gain.shape[0]
    where = jnp.stack([lax.axis_index(a) for a in TP]).astype(jnp.int32)
    gains = norm_gain.reshape(1, model)
    active_row, ids = active.reshape(1, count), expert_ids.T
    sent = pl.pallas_call(
        functools.partial(dispatch_kernel, seat_limit, groups),
        out_shape=jax.ShapeDtypeStruct((groups, seat_limit, width), BF16),
        compiler_params=pltpu.CompilerParams(vmem_limit_bytes=60 * MIB),
    )(ids, active_row, tokens)
    arriving = lax.all_to_all(sent, "expert", split_axis=0, concat_axis=0, tiled=True)
    n = lax.axis_size(TP[0])
    rows = arriving.reshape(CHUNKS, -1, width)
    first = [rows] + [along(rows, 0, k) for k in range(1, n)]
    weights = (gate_weight[0], up_weight[0], down_weight[0])
    owns = []
    for stack in stacked((gains, where), first):
        owns.append([stack] + [along(stack, 1, k) for k in range(1, n)])
    chunks = []
    for own in owns:
        partner = [swapped(a) for a in own]
        keep, send = experts_of(where, own, partner, gains, *weights)
        chunks.append(started(keep, send))
    returning = finished(chunks).reshape(groups, seat_limit, width)
    arrived = lax.all_to_all(returning, "expert", split_axis=0, concat_axis=0, tiled=True)
    return pl.pallas_call(
        functools.partial(combine_kernel, seat_limit, groups),
        out_shape=jax.ShapeDtypeStruct((count, width), BF16),
        compiler_params=pltpu.CompilerParams(vmem_limit_bytes=2 * MIB),
    )(ids, active_row, route_logits.T, arrived)


def solution(mesh):
    split = Mesh(
        mesh.devices.reshape(mesh.shape["expert"], 4, 4, 2), ("expert", "tp_0", "tp_1", "tp_2")
    )
    in_specs = (
        P("expert", TP),
        P(),
        P("expert", None),
        P("expert", None),
        P("expert"),
        P("expert", TP, None),
        P("expert", TP, None),
        P("expert", TP, None),
    )
    out_specs = P("expert", TP)
    return jax.shard_map(local, mesh=split, in_specs=in_specs, out_specs=out_specs, check_vma=False)
```

```python
import functools

import jax
import jax.numpy as jnp
from jax import lax
from jax.experimental import pallas as pl
from jax.experimental.pallas import tpu as pltpu
from jax.sharding import Mesh
from jax.sharding import PartitionSpec as P


TP = ("tp_0", "tp_1", "tp_2")
epsilon = 1e-05
F32, BF16 = jnp.float32, jnp.bfloat16
MIB = 1024 * 1024
CHUNKS = 2
STACK_FLOPS = 5000000000


def moved(array, target):
    nx, ny, cores = (lax.axis_size(a) for a in TP)
    flat = lambda x, y, core: ((x % nx) * ny + y % ny) * cores + core
    pairs = [
        (flat(x, y, core), flat(*target(x, y, core)))
        for x in range(nx)
        for y in range(ny)
        for core in range(cores)
    ]
    return lax.ppermute(array, TP, pairs)


def along(array, stage, step, other=0):
    def target(x, y, core):
        return (x + step, y, core) if core ^ other == stage else (x, y + step, core)

    return moved(array, target)


def swapped(array):
    return moved(array, lambda x, y, core: (x, y, 1 - core))


def column(row):
    count = row.shape[1]
    eye = lax.broadcasted_iota(jnp.int32, (count, count), 0) == lax.broadcasted_iota(jnp.int32, (count, count), 1)
    return jnp.sum(jnp.where(eye, row, jnp.zeros_like(row)), axis=1, keepdims=True)


def seats(ids_ref, active_ref, seat_limit, experts):
    count = ids_ref.shape[1]
    live = column(active_ref[...])
    first, second = column(ids_ref[0:1, :]), column(ids_ref[1:2, :])
    number = lax.broadcasted_iota(jnp.int32, (count, 128), 1)
    named = ((first == number) | (second == number)) & (live > 0)
    earlier = lax.broadcasted_iota(jnp.int32, (count, count), 1) < lax.broadcasted_iota(jnp.int32, (count, count), 0)
    place = jnp.dot(earlier.astype(BF16), named.astype(BF16), preferred_element_type=F32).astype(jnp.int32)
    place = jnp.where(named, place, -1)
    spot = lax.broadcasted_iota(jnp.int32, (count, seat_limit), 1)
    return live, first, second, [place[:, e : e + 1] == spot for e in range(experts)]


def dispatch_kernel(seat_limit, experts, ids_ref, active_ref, tokens_ref, out_ref):
    _, _, _, columns = seats(ids_ref, active_ref, seat_limit, experts)
    rows = tokens_ref[...]
    for e, hot in enumerate(columns):
        picked = lax.dot_general(
            hot.astype(BF16), rows, (((0,), (0,)), ((), ())), preferred_element_type=F32
        )
        out_ref[e] = picked.astype(BF16)


def combine_kernel(seat_limit, experts, ids_ref, active_ref, logits_ref, arrived_ref, out_ref):
    live, first, second, columns = seats(ids_ref, active_ref, seat_limit, experts)
    logits = logits_ref[...]
    raised = jnp.exp(logits - jnp.max(logits, axis=0, keepdims=True))
    probs = raised / jnp.sum(raised, axis=0, keepdims=True)
    total = jnp.zeros(out_ref.shape, F32)
    for k, ids in enumerate((first, second)):
        picked = jnp.zeros(out_ref.shape, F32)
        for e, hot in enumerate(columns):
            mine = (hot & (ids == e)).astype(BF16)
            picked = picked + jnp.dot(mine, arrived_ref[e], preferred_element_type=F32)
        total = total + column(probs[k : k + 1, :]) * live.astype(F32) * picked
    out_ref[...] = total.astype(BF16)


def expert_kernel(n, crossed, where_ref, *refs):
    own, partner = refs[:n], refs[n : 2 * n]
    gain_ref, gate_ref, up_ref, down_ref, keep_ref, send_ref, normed_ref = refs[2 * n :]
    x, y, core = where_ref[0], where_ref[1], where_ref[2]
    rows = normed_ref.shape[0]
    width = own[0].shape[-1]
    squares = jnp.zeros((rows, width), F32)
    for pieces in (own, partner):
        for k2 in range(n):
            for k1 in range(n):
                value = pieces[k2][k1].astype(F32)
                squares = squares + value * value
    mean_square = jnp.sum(squares, axis=1, keepdims=True) / (2 * n * n * width)
    scale = lax.rsqrt(mean_square + epsilon)
    for pieces, parity in ((own, core), (partner, 1 - core)):
        for k2 in range(n):
            for k1 in range(n):
                at_x = lax.rem(x - jnp.where(parity == 0, k1, k2) + n, n)
                at_y = lax.rem(y - jnp.where(parity == 0, k2, k1) + n, n)
                t = (at_x * n + at_y) * 2 + parity
                value = pieces[k2][k1].astype(F32) * scale * gain_ref[:, pl.ds(pl.multiple_of(t * width, width), width)].astype(F32)
                normed_ref[:, pl.ds(pl.multiple_of(t * width, width), width)] = value.astype(BF16)
    normed = normed_ref[...]
    dims = (((1,), (1,)), ((), ()))
    gate = lax.dot_general(normed, gate_ref[...], dims, preferred_element_type=F32)
    up = lax.dot_general(normed, up_ref[...], dims, preferred_element_type=F32)
    hidden = (gate / (1.0 + jnp.exp(-gate)) * up).astype(BF16)
    for dx in range(n):
        for dy in range(n):
            q = lax.rem(x + dx, n) * n + lax.rem(y + dy, n)
            part = down_ref[:, pl.ds(pl.multiple_of(q * 2 * width, 2 * width), 2 * width)]
            both = jnp.dot(hidden, part, preferred_element_type=F32)
            low, high = both[:, :width], both[:, width:]
            if (dx == crossed) == (dy == crossed):
                one, two = jnp.where(core == 0, dx, dy), jnp.where(core == 0, dy, dx)
                kept, sent = (high, low) if dx == crossed else (low, high)
                keep_ref[one, two] = jnp.where(core == 0, kept, sent)
                send_ref[two, one] = jnp.where(core == 0, sent, kept)
                continue
            keeper = 1 if dx == crossed else 0
            for ref, condition in ((keep_ref, core == keeper), (send_ref, core != keeper)):

                @pl.when(condition)
                def _(ref=ref, dx=dx, dy=dy, low=low, high=high):
                    ref[dx, dy] = low
                    ref[dy, dx] = high


def stack_kernel(skipped, *refs):
    refs = refs[skipped:]
    half = len(refs) - CHUNKS
    for chunk, out_ref in enumerate(refs[half:]):
        for k, ref in enumerate(refs[:half]):
            out_ref[k] = ref[chunk]


def stacked(after, pieces):
    out = jax.ShapeDtypeStruct((len(pieces),) + pieces[0].shape[1:], BF16)
    return pl.pallas_call(
        functools.partial(stack_kernel, len(after)),
        out_shape=[out] * CHUNKS,
        in_specs=[pl.BlockSpec(memory_space=pltpu.HBM)] * len(after)
        + [pl.BlockSpec(memory_space=pltpu.VMEM)] * len(pieces),
        out_specs=[pl.BlockSpec(memory_space=pltpu.VMEM)] * CHUNKS,
        compiler_params=pltpu.CompilerParams(vmem_limit_bytes=4 * MIB),
        cost_estimate=pl.CostEstimate(flops=STACK_FLOPS, transcendentals=0, bytes_accessed=0),
    )(*after, *pieces)


def experts_of(crossed, where, own, partner, gains, gate, up, down):
    n = len(own)
    _, rows, width = own[0].shape
    model = gate.shape[1]
    vmem = pl.BlockSpec(memory_space=pltpu.VMEM)
    out = jax.ShapeDtypeStruct((n, n, rows, width), F32)
    return pl.pallas_call(
        functools.partial(expert_kernel, n, crossed),
        out_shape=(out, out),
        in_specs=[pl.BlockSpec(memory_space=pltpu.SMEM)] + [vmem] * (2 * n + 4),
        out_specs=(vmem, vmem),
        scratch_shapes=[pltpu.VMEM((rows, model), BF16)],
        compiler_params=pltpu.CompilerParams(vmem_limit_bytes=10 * MIB),
        cost_estimate=pl.CostEstimate(flops=3000000000, transcendentals=0, bytes_accessed=0),
    )(where, *own, *partner, gains, gate, up, down)


STEPS = 8
TOP = 32000.0
SPARE = 16


def scaled(blocks, refs):
    largest = functools.reduce(jnp.maximum, [jnp.abs(b) for group in blocks for b in group])
    largest = jnp.maximum(jnp.max(largest, axis=1, keepdims=True), 1e-32)
    code = jnp.ceil(STEPS * jnp.log2(largest)) + 1.0
    factor = TOP * jnp.exp2(code * (-1.0 / STEPS))
    rows, width = blocks[0][0].shape
    eye = lax.broadcasted_iota(jnp.int32, (width, width), 0) == lax.broadcasted_iota(jnp.int32, (width, width), 1)
    line = lax.broadcasted_iota(jnp.int32, (SPARE, width), 0)
    tile = jnp.zeros((SPARE, width), F32)
    for g in range(rows // width):
        part = jnp.sum(jnp.where(eye, code[g * width : (g + 1) * width], 0.0), axis=0, keepdims=True)
        tile = jnp.where(line == g, part, tile)
    for group, ref in zip(blocks, refs):
        for i, b in enumerate(group):
            ref[pl.ds(i * rows, rows), :] = jnp.round(b * factor).astype(jnp.int32).astype(jnp.int16)
        ref[pl.ds(len(group) * rows, SPARE), :] = tile.astype(jnp.int32).astype(jnp.int16)


def factors(ref, count, rows):
    tile = ref[pl.ds(count * rows, SPARE), :].astype(jnp.int32).astype(F32)
    width = tile.shape[1]
    code = jnp.concatenate([column(tile[g : g + 1, :]) for g in range(rows // width)], axis=0)
    return jnp.exp2(code * (1.0 / STEPS)) * (1.0 / TOP)


def widened(ref, i, rows):
    return ref[pl.ds(i * rows, rows), :].astype(jnp.int32).astype(F32)


def first_kernel(keep_ref, got_ref, own_ref, *out_refs):
    n = keep_ref.shape[0]
    for k2 in range(n):
        own_ref[k2] = keep_ref[0, k2] + got_ref[0, k2]
    blocks = [[keep_ref[k1, k2] + got_ref[k1, k2] for k2 in range(n)] for k1 in range(1, n)]
    scaled(blocks, out_refs)


def second_kernel(chunks, *refs):
    ins, sum_ref, out_refs = refs[: 4 * chunks], refs[4 * chunks], refs[4 * chunks + 1 :]
    n, rows, _ = ins[0].shape
    totals = []
    for chunk in range(chunks):
        own_ref, *got_refs = ins[4 * chunk : 4 * chunk + 4]
        by = [factors(got, n, rows) for got in got_refs]
        totals.append([])
        for k2 in range(n):
            total = own_ref[k2]
            for got, factor in zip(got_refs, by):
                total = total + widened(got, k2, rows) * factor
            totals[-1].append(total)
    totals = [jnp.concatenate(parts, axis=0) for parts in zip(*totals)]
    sum_ref[...] = totals[0]
    scaled([[total] for total in totals[1:]], out_refs)


def third_kernel(own_ref, *refs):
    got_refs, out_ref = refs[:-1], refs[-1]
    rows, _ = own_ref.shape
    total = own_ref[...]
    for got in got_refs:
        total = total + widened(got, 0, rows) * factors(got, 1, rows)
    out_ref[...] = total.astype(BF16)


def coded(blocks, rows, width):
    return jax.ShapeDtypeStruct((blocks * rows + SPARE, width), jnp.int16)


def started(crossed, keep, send):
    n, _, rows, width = keep.shape
    got = swapped(send)
    own, *parts = pl.pallas_call(
        first_kernel,
        out_shape=[jax.ShapeDtypeStruct((n, rows, width), F32)] + [coded(n, rows, width)] * (n - 1),
        compiler_params=pltpu.CompilerParams(vmem_limit_bytes=8 * MIB),
    )(keep, got)
    for step in range(1, n):
        parts[step - 1] = along(parts[step - 1], 0, step, int(step == crossed))
        if step == crossed:
            parts[step - 1] = swapped(parts[step - 1])
    return [own] + parts


def finished(chunks):
    n, rows, width = chunks[0][0].shape
    rows = rows * len(chunks)
    own, *parts = pl.pallas_call(
        functools.partial(second_kernel, len(chunks)),
        out_shape=[jax.ShapeDtypeStruct((rows, width), F32)] + [coded(1, rows, width)] * (n - 1),
        compiler_params=pltpu.CompilerParams(vmem_limit_bytes=4 * MIB),
    )(*[a for chunk in chunks for a in chunk])
    parts = [along(part, 1, k + 1) for k, part in enumerate(parts)]
    return pl.pallas_call(
        third_kernel,
        out_shape=jax.ShapeDtypeStruct((rows, width), BF16),
        compiler_params=pltpu.CompilerParams(vmem_limit_bytes=2 * MIB),
    )(own, *parts)


def local(tokens, norm_gain, route_logits, expert_ids, active, gate_weight, up_weight, down_weight):
    groups = lax.axis_size("expert")
    count, width = tokens.shape
    seat_limit = count // 2
    model = norm_gain.shape[0]
    where = jnp.stack([lax.axis_index(a) for a in TP]).astype(jnp.int32)
    gains = norm_gain.reshape(1, model)
    active_row, ids = active.reshape(1, count), expert_ids.T
    sent = pl.pallas_call(
        functools.partial(dispatch_kernel, seat_limit, groups),
        out_shape=jax.ShapeDtypeStruct((groups, seat_limit, width), BF16),
        compiler_params=pltpu.CompilerParams(vmem_limit_bytes=60 * MIB),
    )(ids, active_row, tokens)
    arriving = lax.all_to_all(sent, "expert", split_axis=0, concat_axis=0, tiled=True)
    n = lax.axis_size(TP[0])
    rows = arriving.reshape(CHUNKS, -1, width)
    first = [rows] + [along(rows, 0, k) for k in range(1, n)]
    weights = (gate_weight[0], up_weight[0], down_weight[0])
    owns = []
    for stack in stacked((gains, where), first):
        owns.append([stack] + [along(stack, 1, k) for k in range(1, n)])
    chunks = []
    for chunk, own in enumerate(owns):
        partner = [swapped(a) for a in own]
        crossed = n // 2 if chunk % 2 else None
        keep, send = experts_of(crossed, where, own, partner, gains, *weights)
        chunks.append(started(crossed, keep, send))
    returning = finished(chunks).reshape(groups, seat_limit, width)
    arrived = lax.all_to_all(returning, "expert", split_axis=0, concat_axis=0, tiled=True)
    return pl.pallas_call(
        functools.partial(combine_kernel, seat_limit, groups),
        out_shape=jax.ShapeDtypeStruct((count, width), BF16),
        compiler_params=pltpu.CompilerParams(vmem_limit_bytes=2 * MIB),
    )(ids, active_row, route_logits.T, arrived)


def solution(mesh):
    split = Mesh(
        mesh.devices.reshape(mesh.shape["expert"], 4, 4, 2), ("expert", "tp_0", "tp_1", "tp_2")
    )
    in_specs = (
        P("expert", TP),
        P(),
        P("expert", None),
        P("expert", None),
        P("expert"),
        P("expert", TP, None),
        P("expert", TP, None),
        P("expert", TP, None),
    )
    out_specs = P("expert", TP)
    return jax.shard_map(local, mesh=split, in_specs=in_specs, out_specs=out_specs, check_vma=False)
```

```python
import functools

import jax
import jax.numpy as jnp
from jax import lax
from jax.experimental import pallas as pl
from jax.experimental.pallas import tpu as pltpu
from jax.sharding import Mesh
from jax.sharding import PartitionSpec as P


TP = ("tp_0", "tp_1", "tp_2")
epsilon = 1e-05
F32, BF16 = jnp.float32, jnp.bfloat16
MIB = 1024 * 1024
CHUNKS = 2
BLOCK = 64
STACK_FLOPS = 5000000000


def moved(array, target):
    nx, ny, cores = (lax.axis_size(a) for a in TP)
    flat = lambda x, y, core: ((x % nx) * ny + y % ny) * cores + core
    pairs = [
        (flat(x, y, core), flat(*target(x, y, core)))
        for x in range(nx)
        for y in range(ny)
        for core in range(cores)
    ]
    return lax.ppermute(array, TP, pairs)


def along(array, stage, step):
    def target(x, y, core):
        return (x + step, y, core) if core == stage else (x, y + step, core)

    return moved(array, target)


def swapped(array):
    return moved(array, lambda x, y, core: (x, y, 1 - core))


def column(row):
    count = row.shape[1]
    eye = lax.broadcasted_iota(jnp.int32, (count, count), 0) == lax.broadcasted_iota(jnp.int32, (count, count), 1)
    return jnp.sum(jnp.where(eye, row, jnp.zeros_like(row)), axis=1, keepdims=True)


def seats(ids_ref, active_ref, seat_limit, experts):
    count = ids_ref.shape[1]
    live = column(active_ref[...])
    first, second = column(ids_ref[0:1, :]), column(ids_ref[1:2, :])
    number = lax.broadcasted_iota(jnp.int32, (count, 128), 1)
    named = ((first == number) | (second == number)) & (live > 0)
    earlier = lax.broadcasted_iota(jnp.int32, (count, count), 1) < lax.broadcasted_iota(jnp.int32, (count, count), 0)
    place = jnp.dot(earlier.astype(BF16), named.astype(BF16), preferred_element_type=F32).astype(jnp.int32)
    place = jnp.where(named, place, -1)
    spot = lax.broadcasted_iota(jnp.int32, (count, seat_limit), 1)
    return live, first, second, [place[:, e : e + 1] == spot for e in range(experts)]


def dispatch_kernel(seat_limit, experts, ids_ref, active_ref, tokens_ref, out_ref):
    _, _, _, columns = seats(ids_ref, active_ref, seat_limit, experts)
    rows = tokens_ref[...]
    for e, hot in enumerate(columns):
        picked = lax.dot_general(
            hot.astype(BF16), rows, (((0,), (0,)), ((), ())), preferred_element_type=F32
        )
        out_ref[e] = picked.astype(BF16)


def combine_kernel(seat_limit, experts, ids_ref, active_ref, logits_ref, arrived_ref, out_ref):
    live, first, second, columns = seats(ids_ref, active_ref, seat_limit, experts)
    logits = logits_ref[...]
    raised = jnp.exp(logits - jnp.max(logits, axis=0, keepdims=True))
    probs = raised / jnp.sum(raised, axis=0, keepdims=True)
    total = jnp.zeros(out_ref.shape, F32)
    for k, ids in enumerate((first, second)):
        picked = jnp.zeros(out_ref.shape, F32)
        for e, hot in enumerate(columns):
            mine = (hot & (ids == e)).astype(BF16)
            picked = picked + jnp.dot(mine, arrived_ref[e], preferred_element_type=F32)
        total = total + column(probs[k : k + 1, :]) * live.astype(F32) * picked
    out_ref[...] = total.astype(BF16)


def expert_kernel(n, where_ref, *refs):
    own, partner = refs[:n], refs[n : 2 * n]
    gain_ref, gate_ref, up_ref, down_ref, keep_ref, send_ref, normed_ref = refs[2 * n :]
    x, y, core = where_ref[0], where_ref[1], where_ref[2]
    rows = normed_ref.shape[0]
    width = own[0].shape[-1]

    def normalize(i, _):
        span = pl.ds(pl.multiple_of(i * BLOCK, BLOCK), BLOCK)
        squares = jnp.zeros((BLOCK, width), F32)
        for pieces in (own, partner):
            for k2 in range(n):
                for k1 in range(n):
                    value = pieces[k2][k1, span, :].astype(F32)
                    squares = squares + value * value
        mean_square = jnp.sum(squares, axis=1, keepdims=True) / (2 * n * n * width)
        scale = lax.rsqrt(mean_square + epsilon)
        for pieces, parity in ((own, core), (partner, 1 - core)):
            for k2 in range(n):
                for k1 in range(n):
                    at_x = lax.rem(x - jnp.where(parity == 0, k1, k2) + n, n)
                    at_y = lax.rem(y - jnp.where(parity == 0, k2, k1) + n, n)
                    t = (at_x * n + at_y) * 2 + parity
                    at = pl.ds(pl.multiple_of(t * width, width), width)
                    value = pieces[k2][k1, span, :].astype(F32) * scale * gain_ref[:, at].astype(F32)
                    normed_ref[span, at] = value.astype(BF16)
        return 0

    lax.fori_loop(0, rows // BLOCK, normalize, 0)
    normed = normed_ref[...]
    dims = (((1,), (1,)), ((), ()))
    gate = lax.dot_general(normed, gate_ref[...], dims, preferred_element_type=F32)
    up = lax.dot_general(normed, up_ref[...], dims, preferred_element_type=F32)
    hidden = (gate / (1.0 + jnp.exp(-gate)) * up).astype(BF16)

    def project(dx, _):
        for dy in range(n):
            q = lax.rem(x + dx, n) * n + lax.rem(y + dy, n)
            part = down_ref[:, pl.ds(pl.multiple_of(q * 2 * width, 2 * width), 2 * width)]
            both = jnp.dot(hidden, part, preferred_element_type=F32)
            low, high = both[:, :width], both[:, width:]
            one, two = jnp.where(core == 0, dx, dy), jnp.where(core == 0, dy, dx)
            keep_ref[one, two] = jnp.where(core == 0, low, high)
            send_ref[two, one] = jnp.where(core == 0, high, low)
        return 0

    lax.fori_loop(0, n, project, 0)


def stack_kernel(skipped, *refs):
    refs = refs[skipped:]
    half = len(refs) - CHUNKS
    for chunk, out_ref in enumerate(refs[half:]):
        for k, ref in enumerate(refs[:half]):
            out_ref[k] = ref[chunk]


def stacked(after, pieces):
    out = jax.ShapeDtypeStruct((len(pieces),) + pieces[0].shape[1:], BF16)
    return pl.pallas_call(
        functools.partial(stack_kernel, len(after)),
        out_shape=[out] * CHUNKS,
        in_specs=[pl.BlockSpec(memory_space=pltpu.HBM)] * len(after)
        + [pl.BlockSpec(memory_space=pltpu.VMEM)] * len(pieces),
        out_specs=[pl.BlockSpec(memory_space=pltpu.VMEM)] * CHUNKS,
        compiler_params=pltpu.CompilerParams(vmem_limit_bytes=4 * MIB),
        cost_estimate=pl.CostEstimate(flops=STACK_FLOPS, transcendentals=0, bytes_accessed=0),
    )(*after, *pieces)


def experts_of(where, own, partner, gains, gate, up, down):
    n = len(own)
    _, rows, width = own[0].shape
    model = gate.shape[1]
    vmem = pl.BlockSpec(memory_space=pltpu.VMEM)
    out = jax.ShapeDtypeStruct((n, n, rows, width), F32)
    return pl.pallas_call(
        functools.partial(expert_kernel, n),
        out_shape=(out, out),
        in_specs=[pl.BlockSpec(memory_space=pltpu.SMEM)] + [vmem] * (2 * n + 4),
        out_specs=(vmem, vmem),
        scratch_shapes=[pltpu.VMEM((rows, model), BF16)],
        compiler_params=pltpu.CompilerParams(vmem_limit_bytes=10 * MIB),
        cost_estimate=pl.CostEstimate(flops=3000000000, transcendentals=0, bytes_accessed=0),
    )(where, *own, *partner, gains, gate, up, down)


STEPS = 8
TOP = 32000.0
SPARE = 16


def scaled(blocks, refs):
    largest = functools.reduce(jnp.maximum, [jnp.abs(b) for group in blocks for b in group])
    largest = jnp.maximum(jnp.max(largest, axis=1, keepdims=True), 1e-32)
    code = jnp.ceil(STEPS * jnp.log2(largest)) + 1.0
    factor = TOP * jnp.exp2(code * (-1.0 / STEPS))
    rows, width = blocks[0][0].shape
    eye = lax.broadcasted_iota(jnp.int32, (width, width), 0) == lax.broadcasted_iota(jnp.int32, (width, width), 1)
    line = lax.broadcasted_iota(jnp.int32, (SPARE, width), 0)
    tile = jnp.zeros((SPARE, width), F32)
    for g in range(rows // width):
        part = jnp.sum(jnp.where(eye, code[g * width : (g + 1) * width], 0.0), axis=0, keepdims=True)
        tile = jnp.where(line == g, part, tile)
    for group, ref in zip(blocks, refs):
        for i, b in enumerate(group):
            ref[pl.ds(i * rows, rows), :] = jnp.round(b * factor).astype(jnp.int32).astype(jnp.int16)
        ref[pl.ds(len(group) * rows, SPARE), :] = tile.astype(jnp.int32).astype(jnp.int16)


def factors(ref, count, rows):
    tile = ref[pl.ds(count * rows, SPARE), :].astype(jnp.int32).astype(F32)
    width = tile.shape[1]
    code = jnp.concatenate([column(tile[g : g + 1, :]) for g in range(rows // width)], axis=0)
    return jnp.exp2(code * (1.0 / STEPS)) * (1.0 / TOP)


def widened(ref, i, rows):
    return ref[pl.ds(i * rows, rows), :].astype(jnp.int32).astype(F32)


def first_kernel(keep_ref, got_ref, own_ref, *out_refs):
    n = keep_ref.shape[0]
    for k2 in range(n):
        own_ref[k2] = keep_ref[0, k2] + got_ref[0, k2]
    blocks = [[keep_ref[k1, k2] + got_ref[k1, k2] for k2 in range(n)] for k1 in range(1, n)]
    scaled(blocks, out_refs)


def second_kernel(chunks, *refs):
    ins, sum_ref, out_refs = refs[: 4 * chunks], refs[4 * chunks], refs[4 * chunks + 1 :]
    n, rows, _ = ins[0].shape
    totals = []
    for chunk in range(chunks):
        own_ref, *got_refs = ins[4 * chunk : 4 * chunk + 4]
        by = [factors(got, n, rows) for got in got_refs]
        totals.append([])
        for k2 in range(n):
            total = own_ref[k2]
            for got, factor in zip(got_refs, by):
                total = total + widened(got, k2, rows) * factor
            totals[-1].append(total)
    totals = [jnp.concatenate(parts, axis=0) for parts in zip(*totals)]
    sum_ref[...] = totals[0]
    scaled([[total] for total in totals[1:]], out_refs)


def third_kernel(own_ref, *refs):
    got_refs, out_ref = refs[:-1], refs[-1]
    rows, _ = own_ref.shape
    total = own_ref[...]
    for got in got_refs:
        total = total + widened(got, 0, rows) * factors(got, 1, rows)
    out_ref[...] = total.astype(BF16)


def coded(blocks, rows, width):
    return jax.ShapeDtypeStruct((blocks * rows + SPARE, width), jnp.int16)


def started(keep, send):
    n, _, rows, width = keep.shape
    own, *parts = pl.pallas_call(
        first_kernel,
        out_shape=[jax.ShapeDtypeStruct((n, rows, width), F32)] + [coded(n, rows, width)] * (n - 1),
        compiler_params=pltpu.CompilerParams(vmem_limit_bytes=8 * MIB),
    )(keep, swapped(send))
    return [own] + [along(part, 0, k + 1) for k, part in enumerate(parts)]


def finished(chunks):
    n, rows, width = chunks[0][0].shape
    rows = rows * len(chunks)
    own, *parts = pl.pallas_call(
        functools.partial(second_kernel, len(chunks)),
        out_shape=[jax.ShapeDtypeStruct((rows, width), F32)] + [coded(1, rows, width)] * (n - 1),
        compiler_params=pltpu.CompilerParams(vmem_limit_bytes=4 * MIB),
    )(*[a for chunk in chunks for a in chunk])
    parts = [along(part, 1, k + 1) for k, part in enumerate(parts)]
    return pl.pallas_call(
        third_kernel,
        out_shape=jax.ShapeDtypeStruct((rows, width), BF16),
        compiler_params=pltpu.CompilerParams(vmem_limit_bytes=2 * MIB),
    )(own, *parts)


def local(tokens, norm_gain, route_logits, expert_ids, active, gate_weight, up_weight, down_weight):
    groups = lax.axis_size("expert")
    count, width = tokens.shape
    seat_limit = count // 2
    model = norm_gain.shape[0]
    where = jnp.stack([lax.axis_index(a) for a in TP]).astype(jnp.int32)
    gains = norm_gain.reshape(1, model)
    active_row, ids = active.reshape(1, count), expert_ids.T
    sent = pl.pallas_call(
        functools.partial(dispatch_kernel, seat_limit, groups),
        out_shape=jax.ShapeDtypeStruct((groups, seat_limit, width), BF16),
        compiler_params=pltpu.CompilerParams(vmem_limit_bytes=60 * MIB),
    )(ids, active_row, tokens)
    arriving = lax.all_to_all(sent, "expert", split_axis=0, concat_axis=0, tiled=True)
    n = lax.axis_size(TP[0])
    rows = arriving.reshape(CHUNKS, -1, width)
    first = [rows] + [along(rows, 0, k) for k in range(1, n)]
    weights = (gate_weight[0], up_weight[0], down_weight[0])
    owns = []
    for stack in stacked((gains, where), first):
        owns.append([stack] + [along(stack, 1, k) for k in range(1, n)])
    chunks = []
    for own in owns:
        partner = [swapped(a) for a in own]
        keep, send = experts_of(where, own, partner, gains, *weights)
        chunks.append(started(keep, send))
    returning = finished(chunks).reshape(groups, seat_limit, width)
    arrived = lax.all_to_all(returning, "expert", split_axis=0, concat_axis=0, tiled=True)
    return pl.pallas_call(
        functools.partial(combine_kernel, seat_limit, groups),
        out_shape=jax.ShapeDtypeStruct((count, width), BF16),
        compiler_params=pltpu.CompilerParams(vmem_limit_bytes=2 * MIB),
    )(ids, active_row, route_logits.T, arrived)


def solution(mesh):
    split = Mesh(
        mesh.devices.reshape(mesh.shape["expert"], 4, 4, 2), ("expert", "tp_0", "tp_1", "tp_2")
    )
    in_specs = (
        P("expert", TP),
        P(),
        P("expert", None),
        P("expert", None),
        P("expert"),
        P("expert", TP, None),
        P("expert", TP, None),
        P("expert", TP, None),
    )
    out_specs = P("expert", TP)
    return jax.shard_map(local, mesh=split, in_specs=in_specs, out_specs=out_specs, check_vma=False)
```

```python
import functools

import jax
import jax.numpy as jnp
from jax import lax
from jax.experimental import pallas as pl
from jax.experimental.pallas import tpu as pltpu
from jax.sharding import Mesh
from jax.sharding import PartitionSpec as P


TP = ("tp_0", "tp_1", "tp_2")
epsilon = 1e-05
F32, BF16 = jnp.float32, jnp.bfloat16
MIB = 1024 * 1024
CHUNKS = 2
STACK_FLOPS = 5000000000


def moved(array, target):
    nx, ny, cores = (lax.axis_size(a) for a in TP)
    flat = lambda x, y, core: ((x % nx) * ny + y % ny) * cores + core
    pairs = [
        (flat(x, y, core), flat(*target(x, y, core)))
        for x in range(nx)
        for y in range(ny)
        for core in range(cores)
    ]
    return lax.ppermute(array, TP, pairs)


def along(array, stage, step):
    def target(x, y, core):
        return (x + step, y, core) if core == stage else (x, y + step, core)

    return moved(array, target)


def swapped(array):
    return moved(array, lambda x, y, core: (x, y, 1 - core))


def column(row):
    count = row.shape[1]
    eye = lax.broadcasted_iota(jnp.int32, (count, count), 0) == lax.broadcasted_iota(jnp.int32, (count, count), 1)
    return jnp.sum(jnp.where(eye, row, jnp.zeros_like(row)), axis=1, keepdims=True)


def seats(ids_ref, active_ref, seat_limit, experts):
    count = ids_ref.shape[1]
    live = column(active_ref[...])
    first, second = column(ids_ref[0:1, :]), column(ids_ref[1:2, :])
    number = lax.broadcasted_iota(jnp.int32, (count, 128), 1)
    named = ((first == number) | (second == number)) & (live > 0)
    earlier = lax.broadcasted_iota(jnp.int32, (count, count), 1) < lax.broadcasted_iota(jnp.int32, (count, count), 0)
    place = jnp.dot(earlier.astype(BF16), named.astype(BF16), preferred_element_type=F32).astype(jnp.int32)
    place = jnp.where(named, place, -1)
    spot = lax.broadcasted_iota(jnp.int32, (count, seat_limit), 1)
    return live, first, second, [place[:, e : e + 1] == spot for e in range(experts)]


def dispatch_kernel(seat_limit, experts, ids_ref, active_ref, tokens_ref, out_ref):
    _, _, _, columns = seats(ids_ref, active_ref, seat_limit, experts)
    rows = tokens_ref[...]
    for e, hot in enumerate(columns):
        picked = lax.dot_general(
            hot.astype(BF16), rows, (((0,), (0,)), ((), ())), preferred_element_type=F32
        )
        out_ref[e] = picked.astype(BF16)


def combine_kernel(seat_limit, experts, ids_ref, active_ref, logits_ref, arrived_ref, out_ref):
    live, first, second, columns = seats(ids_ref, active_ref, seat_limit, experts)
    logits = logits_ref[...]
    raised = jnp.exp(logits - jnp.max(logits, axis=0, keepdims=True))
    probs = raised / jnp.sum(raised, axis=0, keepdims=True)
    total = jnp.zeros(out_ref.shape, F32)
    for k, ids in enumerate((first, second)):
        picked = jnp.zeros(out_ref.shape, F32)
        for e, hot in enumerate(columns):
            mine = (hot & (ids == e)).astype(BF16)
            picked = picked + jnp.dot(mine, arrived_ref[e], preferred_element_type=F32)
        total = total + column(probs[k : k + 1, :]) * live.astype(F32) * picked
    out_ref[...] = total.astype(BF16)


def expert_kernel(n, where_ref, *refs):
    own, partner = refs[:n], refs[n : 2 * n]
    gain_ref, gate_ref, up_ref, down_ref, keep_ref, send_ref = refs[2 * n :]
    x, y, core = where_ref[0], where_ref[1], where_ref[2]
    rows, width = own[0].shape[1:]
    squares = jnp.zeros((rows, width), F32)
    for pieces in (own, partner):
        for k2 in range(n):
            for k1 in range(n):
                value = pieces[k2][k1].astype(F32)
                squares = squares + value * value
    mean_square = jnp.sum(squares, axis=1, keepdims=True) / (2 * n * n * width)
    scale = lax.rsqrt(mean_square + epsilon)
    dims = (((1,), (1,)), ((), ()))
    gate = up = None
    for k1 in range(n):
        for k2 in range(n):
            at_x = lax.rem(x - jnp.where(core == 0, k1, k2) + n, n)
            at_y = lax.rem(y - jnp.where(core == 0, k2, k1) + n, n)
            at = pl.ds(pl.multiple_of((at_x * n + at_y) * 2 * width, 2 * width), 2 * width)
            mine, other = own[k2][k1], partner[k1][k2]
            pair = [jnp.where(core == 0, mine, other), jnp.where(core == 0, other, mine)]
            value = jnp.concatenate(pair, axis=1).astype(F32) * scale * gain_ref[:, at].astype(F32)
            value = value.astype(BF16)
            gate_part = lax.dot_general(value, gate_ref[:, at], dims, preferred_element_type=F32)
            up_part = lax.dot_general(value, up_ref[:, at], dims, preferred_element_type=F32)
            gate = gate_part if gate is None else gate + gate_part
            up = up_part if up is None else up + up_part
    hidden = (gate / (1.0 + jnp.exp(-gate)) * up).astype(BF16)
    for dx in range(n):
        for dy in range(n):
            q = lax.rem(x + dx, n) * n + lax.rem(y + dy, n)
            part = down_ref[:, pl.ds(pl.multiple_of(q * 2 * width, 2 * width), 2 * width)]
            both = jnp.dot(hidden, part, preferred_element_type=F32)
            low, high = both[:, :width], both[:, width:]
            one, two = jnp.where(core == 0, dx, dy), jnp.where(core == 0, dy, dx)
            keep_ref[one, two] = jnp.where(core == 0, low, high)
            send_ref[two, one] = jnp.where(core == 0, high, low)


def stack_kernel(skipped, *refs):
    refs = refs[skipped:]
    half = len(refs) - CHUNKS
    for chunk, out_ref in enumerate(refs[half:]):
        for k, ref in enumerate(refs[:half]):
            out_ref[k] = ref[chunk]


def stacked(after, pieces):
    out = jax.ShapeDtypeStruct((len(pieces),) + pieces[0].shape[1:], BF16)
    return pl.pallas_call(
        functools.partial(stack_kernel, len(after)),
        out_shape=[out] * CHUNKS,
        in_specs=[pl.BlockSpec(memory_space=pltpu.HBM)] * len(after)
        + [pl.BlockSpec(memory_space=pltpu.VMEM)] * len(pieces),
        out_specs=[pl.BlockSpec(memory_space=pltpu.VMEM)] * CHUNKS,
        compiler_params=pltpu.CompilerParams(vmem_limit_bytes=4 * MIB),
        cost_estimate=pl.CostEstimate(flops=STACK_FLOPS, transcendentals=0, bytes_accessed=0),
    )(*after, *pieces)


def experts_of(where, own, partner, gains, gate, up, down):
    n = len(own)
    _, rows, width = own[0].shape
    vmem = pl.BlockSpec(memory_space=pltpu.VMEM)
    out = jax.ShapeDtypeStruct((n, n, rows, width), F32)
    return pl.pallas_call(
        functools.partial(expert_kernel, n),
        out_shape=(out, out),
        in_specs=[pl.BlockSpec(memory_space=pltpu.SMEM)] + [vmem] * (2 * n + 4),
        out_specs=(vmem, vmem),
        compiler_params=pltpu.CompilerParams(vmem_limit_bytes=10 * MIB),
        cost_estimate=pl.CostEstimate(flops=3000000000, transcendentals=0, bytes_accessed=0),
    )(where, *own, *partner, gains, gate, up, down)


STEPS = 8
TOP = 32000.0
SPARE = 16


def scaled(blocks, refs):
    largest = functools.reduce(jnp.maximum, [jnp.abs(b) for group in blocks for b in group])
    largest = jnp.maximum(jnp.max(largest, axis=1, keepdims=True), 1e-32)
    code = jnp.ceil(STEPS * jnp.log2(largest)) + 1.0
    factor = TOP * jnp.exp2(code * (-1.0 / STEPS))
    rows, width = blocks[0][0].shape
    eye = lax.broadcasted_iota(jnp.int32, (width, width), 0) == lax.broadcasted_iota(jnp.int32, (width, width), 1)
    line = lax.broadcasted_iota(jnp.int32, (SPARE, width), 0)
    tile = jnp.zeros((SPARE, width), F32)
    for g in range(rows // width):
        part = jnp.sum(jnp.where(eye, code[g * width : (g + 1) * width], 0.0), axis=0, keepdims=True)
        tile = jnp.where(line == g, part, tile)
    for group, ref in zip(blocks, refs):
        for i, b in enumerate(group):
            ref[pl.ds(i * rows, rows), :] = jnp.round(b * factor).astype(jnp.int32).astype(jnp.int16)
        ref[pl.ds(len(group) * rows, SPARE), :] = tile.astype(jnp.int32).astype(jnp.int16)


def factors(ref, count, rows):
    tile = ref[pl.ds(count * rows, SPARE), :].astype(jnp.int32).astype(F32)
    width = tile.shape[1]
    code = jnp.concatenate([column(tile[g : g + 1, :]) for g in range(rows // width)], axis=0)
    return jnp.exp2(code * (1.0 / STEPS)) * (1.0 / TOP)


def widened(ref, i, rows):
    return ref[pl.ds(i * rows, rows), :].astype(jnp.int32).astype(F32)


def first_kernel(keep_ref, got_ref, own_ref, *out_refs):
    n = keep_ref.shape[0]
    for k2 in range(n):
        own_ref[k2] = keep_ref[0, k2] + got_ref[0, k2]
    blocks = [[keep_ref[k1, k2] + got_ref[k1, k2] for k2 in range(n)] for k1 in range(1, n)]
    scaled(blocks, out_refs)


def second_kernel(chunks, *refs):
    ins, sum_ref, out_refs = refs[: 4 * chunks], refs[4 * chunks], refs[4 * chunks + 1 :]
    n, rows, _ = ins[0].shape
    totals = []
    for chunk in range(chunks):
        own_ref, *got_refs = ins[4 * chunk : 4 * chunk + 4]
        by = [factors(got, n, rows) for got in got_refs]
        totals.append([])
        for k2 in range(n):
            total = own_ref[k2]
            for got, factor in zip(got_refs, by):
                total = total + widened(got, k2, rows) * factor
            totals[-1].append(total)
    totals = [jnp.concatenate(parts, axis=0) for parts in zip(*totals)]
    sum_ref[...] = totals[0]
    scaled([[total] for total in totals[1:]], out_refs)


def third_kernel(own_ref, *refs):
    got_refs, out_ref = refs[:-1], refs[-1]
    rows, _ = own_ref.shape
    total = own_ref[...]
    for got in got_refs:
        total = total + widened(got, 0, rows) * factors(got, 1, rows)
    out_ref[...] = total.astype(BF16)


def coded(blocks, rows, width):
    return jax.ShapeDtypeStruct((blocks * rows + SPARE, width), jnp.int16)


def started(keep, send):
    n, _, rows, width = keep.shape
    own, *parts = pl.pallas_call(
        first_kernel,
        out_shape=[jax.ShapeDtypeStruct((n, rows, width), F32)] + [coded(n, rows, width)] * (n - 1),
        compiler_params=pltpu.CompilerParams(vmem_limit_bytes=8 * MIB),
    )(keep, swapped(send))
    return [own] + [along(part, 0, k + 1) for k, part in enumerate(parts)]


def finished(chunks):
    n, rows, width = chunks[0][0].shape
    rows = rows * len(chunks)
    own, *parts = pl.pallas_call(
        functools.partial(second_kernel, len(chunks)),
        out_shape=[jax.ShapeDtypeStruct((rows, width), F32)] + [coded(1, rows, width)] * (n - 1),
        compiler_params=pltpu.CompilerParams(vmem_limit_bytes=4 * MIB),
    )(*[a for chunk in chunks for a in chunk])
    parts = [along(part, 1, k + 1) for k, part in enumerate(parts)]
    return pl.pallas_call(
        third_kernel,
        out_shape=jax.ShapeDtypeStruct((rows, width), BF16),
        compiler_params=pltpu.CompilerParams(vmem_limit_bytes=2 * MIB),
    )(own, *parts)


def local(tokens, norm_gain, route_logits, expert_ids, active, gate_weight, up_weight, down_weight):
    groups = lax.axis_size("expert")
    count, width = tokens.shape
    seat_limit = count // 2
    model = norm_gain.shape[0]
    where = jnp.stack([lax.axis_index(a) for a in TP]).astype(jnp.int32)
    gains = norm_gain.reshape(1, model)
    active_row, ids = active.reshape(1, count), expert_ids.T
    sent = pl.pallas_call(
        functools.partial(dispatch_kernel, seat_limit, groups),
        out_shape=jax.ShapeDtypeStruct((groups, seat_limit, width), BF16),
        compiler_params=pltpu.CompilerParams(vmem_limit_bytes=60 * MIB),
    )(ids, active_row, tokens)
    arriving = lax.all_to_all(sent, "expert", split_axis=0, concat_axis=0, tiled=True)
    n = lax.axis_size(TP[0])
    rows = arriving.reshape(CHUNKS, -1, width)
    first = [rows] + [along(rows, 0, k) for k in range(1, n)]
    weights = (gate_weight[0], up_weight[0], down_weight[0])
    owns = []
    for stack in stacked((gains, where), first):
        owns.append([stack] + [along(stack, 1, k) for k in range(1, n)])
    chunks = []
    for own in owns:
        partner = [swapped(a) for a in own]
        keep, send = experts_of(where, own, partner, gains, *weights)
        chunks.append(started(keep, send))
    returning = finished(chunks).reshape(groups, seat_limit, width)
    arrived = lax.all_to_all(returning, "expert", split_axis=0, concat_axis=0, tiled=True)
    return pl.pallas_call(
        functools.partial(combine_kernel, seat_limit, groups),
        out_shape=jax.ShapeDtypeStruct((count, width), BF16),
        compiler_params=pltpu.CompilerParams(vmem_limit_bytes=2 * MIB),
    )(ids, active_row, route_logits.T, arrived)


def solution(mesh):
    split = Mesh(
        mesh.devices.reshape(mesh.shape["expert"], 4, 4, 2), ("expert", "tp_0", "tp_1", "tp_2")
    )
    in_specs = (
        P("expert", TP),
        P(),
        P("expert", None),
        P("expert", None),
        P("expert"),
        P("expert", TP, None),
        P("expert", TP, None),
        P("expert", TP, None),
    )
    out_specs = P("expert", TP)
    return jax.shard_map(local, mesh=split, in_specs=in_specs, out_specs=out_specs, check_vma=False)
```

```python
import functools

import jax
import jax.numpy as jnp
from jax import lax
from jax.experimental import pallas as pl
from jax.experimental.pallas import tpu as pltpu
from jax.sharding import Mesh
from jax.sharding import PartitionSpec as P


TP = ("tp_0", "tp_1", "tp_2")
epsilon = 1e-05
F32, BF16 = jnp.float32, jnp.bfloat16
MIB = 1024 * 1024
CHUNKS = 2
STACK_FLOPS = 5000000000


def moved(array, target):
    nx, ny, cores = (lax.axis_size(a) for a in TP)
    flat = lambda x, y, core: ((x % nx) * ny + y % ny) * cores + core
    pairs = [
        (flat(x, y, core), flat(*target(x, y, core)))
        for x in range(nx)
        for y in range(ny)
        for core in range(cores)
    ]
    return lax.ppermute(array, TP, pairs)


def along(array, stage, step):
    def target(x, y, core):
        return (x + step, y, core) if core == stage else (x, y + step, core)

    return moved(array, target)


def swapped(array):
    return moved(array, lambda x, y, core: (x, y, 1 - core))


def column(row):
    count = row.shape[1]
    eye = lax.broadcasted_iota(jnp.int32, (count, count), 0) == lax.broadcasted_iota(jnp.int32, (count, count), 1)
    return jnp.sum(jnp.where(eye, row, jnp.zeros_like(row)), axis=1, keepdims=True)


def seats(ids_ref, active_ref, seat_limit, experts):
    count = ids_ref.shape[1]
    live = column(active_ref[...])
    first, second = column(ids_ref[0:1, :]), column(ids_ref[1:2, :])
    number = lax.broadcasted_iota(jnp.int32, (count, 128), 1)
    named = ((first == number) | (second == number)) & (live > 0)
    earlier = lax.broadcasted_iota(jnp.int32, (count, count), 1) < lax.broadcasted_iota(jnp.int32, (count, count), 0)
    place = jnp.dot(earlier.astype(BF16), named.astype(BF16), preferred_element_type=F32).astype(jnp.int32)
    place = jnp.where(named, place, -1)
    spot = lax.broadcasted_iota(jnp.int32, (count, seat_limit), 1)
    return live, first, second, [place[:, e : e + 1] == spot for e in range(experts)]


def dispatch_kernel(seat_limit, experts, ids_ref, active_ref, tokens_ref, out_ref):
    _, _, _, columns = seats(ids_ref, active_ref, seat_limit, experts)
    rows = tokens_ref[...]
    for e, hot in enumerate(columns):
        picked = lax.dot_general(
            hot.astype(BF16), rows, (((0,), (0,)), ((), ())), preferred_element_type=F32
        )
        out_ref[e] = picked.astype(BF16)


def combine_kernel(seat_limit, experts, ids_ref, active_ref, logits_ref, arrived_ref, out_ref):
    live, first, second, columns = seats(ids_ref, active_ref, seat_limit, experts)
    logits = logits_ref[...]
    raised = jnp.exp(logits - jnp.max(logits, axis=0, keepdims=True))
    probs = raised / jnp.sum(raised, axis=0, keepdims=True)
    total = jnp.zeros(out_ref.shape, F32)
    for k, ids in enumerate((first, second)):
        picked = jnp.zeros(out_ref.shape, F32)
        for e, hot in enumerate(columns):
            mine = (hot & (ids == e)).astype(BF16)
            picked = picked + jnp.dot(mine, arrived_ref[e], preferred_element_type=F32)
        total = total + column(probs[k : k + 1, :]) * live.astype(F32) * picked
    out_ref[...] = total.astype(BF16)


def expert_kernel(n, where_ref, *refs):
    own, partner = refs[:n], refs[n : 2 * n]
    gain_ref, gate_ref, up_ref, down_ref, keep_ref, send_ref = refs[2 * n :]
    x, y, core = where_ref[0], where_ref[1], where_ref[2]
    rows, width = own[0].shape[1:]
    squares = jnp.zeros((rows, width), F32)
    for pieces in (own, partner):
        for k2 in range(n):
            for k1 in range(n):
                value = pieces[k2][k1].astype(F32)
                squares = squares + value * value
    mean_square = jnp.sum(squares, axis=1, keepdims=True) / (2 * n * n * width)
    scale = lax.rsqrt(mean_square + epsilon)
    dims = (((1,), (1,)), ((), ()))
    gate = up = None
    held = []
    for k1 in range(n):
        for k2 in range(n):
            at_x = lax.rem(x - jnp.where(core == 0, k1, k2) + n, n)
            at_y = lax.rem(y - jnp.where(core == 0, k2, k1) + n, n)
            at = pl.ds(pl.multiple_of((at_x * n + at_y) * 2 * width, 2 * width), 2 * width)
            mine, other = own[k2][k1], partner[k1][k2]
            pair = [jnp.where(core == 0, mine, other), jnp.where(core == 0, other, mine)]
            value = jnp.concatenate(pair, axis=1).astype(F32) * scale * gain_ref[:, at].astype(F32)
            value = value.astype(BF16)
            held.append((value, gate_ref[:, at], up_ref[:, at]))
            if len(held) < 2:
                continue
            value, gate_part, up_part = (jnp.concatenate(parts, axis=1) for parts in zip(*held))
            held = []
            gate_part = lax.dot_general(value, gate_part, dims, preferred_element_type=F32)
            up_part = lax.dot_general(value, up_part, dims, preferred_element_type=F32)
            gate = gate_part if gate is None else gate + gate_part
            up = up_part if up is None else up + up_part
    hidden = (gate / (1.0 + jnp.exp(-gate)) * up).astype(BF16)
    for dx in range(n):
        for dy in range(n):
            q = lax.rem(x + dx, n) * n + lax.rem(y + dy, n)
            part = down_ref[:, pl.ds(pl.multiple_of(q * 2 * width, 2 * width), 2 * width)]
            both = jnp.dot(hidden, part, preferred_element_type=F32)
            low, high = both[:, :width], both[:, width:]
            one, two = jnp.where(core == 0, dx, dy), jnp.where(core == 0, dy, dx)
            keep_ref[one, two] = jnp.where(core == 0, low, high)
            send_ref[two, one] = jnp.where(core == 0, high, low)


def stack_kernel(skipped, *refs):
    refs = refs[skipped:]
    half = len(refs) - CHUNKS
    for chunk, out_ref in enumerate(refs[half:]):
        for k, ref in enumerate(refs[:half]):
            out_ref[k] = ref[chunk]


def stacked(after, pieces):
    out = jax.ShapeDtypeStruct((len(pieces),) + pieces[0].shape[1:], BF16)
    return pl.pallas_call(
        functools.partial(stack_kernel, len(after)),
        out_shape=[out] * CHUNKS,
        in_specs=[pl.BlockSpec(memory_space=pltpu.HBM)] * len(after)
        + [pl.BlockSpec(memory_space=pltpu.VMEM)] * len(pieces),
        out_specs=[pl.BlockSpec(memory_space=pltpu.VMEM)] * CHUNKS,
        compiler_params=pltpu.CompilerParams(vmem_limit_bytes=4 * MIB),
        cost_estimate=pl.CostEstimate(flops=STACK_FLOPS, transcendentals=0, bytes_accessed=0),
    )(*after, *pieces)


def experts_of(where, own, partner, gains, gate, up, down):
    n = len(own)
    _, rows, width = own[0].shape
    vmem = pl.BlockSpec(memory_space=pltpu.VMEM)
    out = jax.ShapeDtypeStruct((n, n, rows, width), F32)
    return pl.pallas_call(
        functools.partial(expert_kernel, n),
        out_shape=(out, out),
        in_specs=[pl.BlockSpec(memory_space=pltpu.SMEM)] + [vmem] * (2 * n + 4),
        out_specs=(vmem, vmem),
        compiler_params=pltpu.CompilerParams(vmem_limit_bytes=10 * MIB),
        cost_estimate=pl.CostEstimate(flops=3000000000, transcendentals=0, bytes_accessed=0),
    )(where, *own, *partner, gains, gate, up, down)


STEPS = 8
TOP = 32000.0
SPARE = 16


def scaled(blocks, refs):
    largest = functools.reduce(jnp.maximum, [jnp.abs(b) for group in blocks for b in group])
    largest = jnp.maximum(jnp.max(largest, axis=1, keepdims=True), 1e-32)
    code = jnp.ceil(STEPS * jnp.log2(largest)) + 1.0
    factor = TOP * jnp.exp2(code * (-1.0 / STEPS))
    rows, width = blocks[0][0].shape
    eye = lax.broadcasted_iota(jnp.int32, (width, width), 0) == lax.broadcasted_iota(jnp.int32, (width, width), 1)
    line = lax.broadcasted_iota(jnp.int32, (SPARE, width), 0)
    tile = jnp.zeros((SPARE, width), F32)
    for g in range(rows // width):
        part = jnp.sum(jnp.where(eye, code[g * width : (g + 1) * width], 0.0), axis=0, keepdims=True)
        tile = jnp.where(line == g, part, tile)
    for group, ref in zip(blocks, refs):
        for i, b in enumerate(group):
            ref[pl.ds(i * rows, rows), :] = jnp.round(b * factor).astype(jnp.int32).astype(jnp.int16)
        ref[pl.ds(len(group) * rows, SPARE), :] = tile.astype(jnp.int32).astype(jnp.int16)


def factors(ref, count, rows):
    tile = ref[pl.ds(count * rows, SPARE), :].astype(jnp.int32).astype(F32)
    width = tile.shape[1]
    code = jnp.concatenate([column(tile[g : g + 1, :]) for g in range(rows // width)], axis=0)
    return jnp.exp2(code * (1.0 / STEPS)) * (1.0 / TOP)


def widened(ref, i, rows):
    return ref[pl.ds(i * rows, rows), :].astype(jnp.int32).astype(F32)


def first_kernel(keep_ref, got_ref, own_ref, *out_refs):
    n = keep_ref.shape[0]
    for k2 in range(n):
        own_ref[k2] = keep_ref[0, k2] + got_ref[0, k2]
    blocks = [[keep_ref[k1, k2] + got_ref[k1, k2] for k2 in range(n)] for k1 in range(1, n)]
    scaled(blocks, out_refs)


def second_kernel(chunks, *refs):
    ins, sum_ref, out_refs = refs[: 4 * chunks], refs[4 * chunks], refs[4 * chunks + 1 :]
    n, rows, _ = ins[0].shape
    totals = []
    for chunk in range(chunks):
        own_ref, *got_refs = ins[4 * chunk : 4 * chunk + 4]
        by = [factors(got, n, rows) for got in got_refs]
        totals.append([])
        for k2 in range(n):
            total = own_ref[k2]
            for got, factor in zip(got_refs, by):
                total = total + widened(got, k2, rows) * factor
            totals[-1].append(total)
    totals = [jnp.concatenate(parts, axis=0) for parts in zip(*totals)]
    sum_ref[...] = totals[0]
    scaled([[total] for total in totals[1:]], out_refs)


def third_kernel(own_ref, *refs):
    got_refs, out_ref = refs[:-1], refs[-1]
    rows, _ = own_ref.shape
    total = own_ref[...]
    for got in got_refs:
        total = total + widened(got, 0, rows) * factors(got, 1, rows)
    out_ref[...] = total.astype(BF16)


def coded(blocks, rows, width):
    return jax.ShapeDtypeStruct((blocks * rows + SPARE, width), jnp.int16)


def started(keep, send):
    n, _, rows, width = keep.shape
    own, *parts = pl.pallas_call(
        first_kernel,
        out_shape=[jax.ShapeDtypeStruct((n, rows, width), F32)] + [coded(n, rows, width)] * (n - 1),
        compiler_params=pltpu.CompilerParams(vmem_limit_bytes=8 * MIB),
    )(keep, swapped(send))
    return [own] + [along(part, 0, k + 1) for k, part in enumerate(parts)]


def finished(chunks):
    n, rows, width = chunks[0][0].shape
    rows = rows * len(chunks)
    own, *parts = pl.pallas_call(
        functools.partial(second_kernel, len(chunks)),
        out_shape=[jax.ShapeDtypeStruct((rows, width), F32)] + [coded(1, rows, width)] * (n - 1),
        compiler_params=pltpu.CompilerParams(vmem_limit_bytes=4 * MIB),
    )(*[a for chunk in chunks for a in chunk])
    parts = [along(part, 1, k + 1) for k, part in enumerate(parts)]
    return pl.pallas_call(
        third_kernel,
        out_shape=jax.ShapeDtypeStruct((rows, width), BF16),
        compiler_params=pltpu.CompilerParams(vmem_limit_bytes=2 * MIB),
    )(own, *parts)


def local(tokens, norm_gain, route_logits, expert_ids, active, gate_weight, up_weight, down_weight):
    groups = lax.axis_size("expert")
    count, width = tokens.shape
    seat_limit = count // 2
    model = norm_gain.shape[0]
    where = jnp.stack([lax.axis_index(a) for a in TP]).astype(jnp.int32)
    gains = norm_gain.reshape(1, model)
    active_row, ids = active.reshape(1, count), expert_ids.T
    sent = pl.pallas_call(
        functools.partial(dispatch_kernel, seat_limit, groups),
        out_shape=jax.ShapeDtypeStruct((groups, seat_limit, width), BF16),
        compiler_params=pltpu.CompilerParams(vmem_limit_bytes=60 * MIB),
    )(ids, active_row, tokens)
    arriving = lax.all_to_all(sent, "expert", split_axis=0, concat_axis=0, tiled=True)
    n = lax.axis_size(TP[0])
    rows = arriving.reshape(CHUNKS, -1, width)
    first = [rows] + [along(rows, 0, k) for k in range(1, n)]
    weights = (gate_weight[0], up_weight[0], down_weight[0])
    owns = []
    for stack in stacked((gains, where), first):
        owns.append([stack] + [along(stack, 1, k) for k in range(1, n)])
    chunks = []
    for own in owns:
        partner = [swapped(a) for a in own]
        keep, send = experts_of(where, own, partner, gains, *weights)
        chunks.append(started(keep, send))
    returning = finished(chunks).reshape(groups, seat_limit, width)
    arrived = lax.all_to_all(returning, "expert", split_axis=0, concat_axis=0, tiled=True)
    return pl.pallas_call(
        functools.partial(combine_kernel, seat_limit, groups),
        out_shape=jax.ShapeDtypeStruct((count, width), BF16),
        compiler_params=pltpu.CompilerParams(vmem_limit_bytes=2 * MIB),
    )(ids, active_row, route_logits.T, arrived)


def solution(mesh):
    split = Mesh(
        mesh.devices.reshape(mesh.shape["expert"], 4, 4, 2), ("expert", "tp_0", "tp_1", "tp_2")
    )
    in_specs = (
        P("expert", TP),
        P(),
        P("expert", None),
        P("expert", None),
        P("expert"),
        P("expert", TP, None),
        P("expert", TP, None),
        P("expert", TP, None),
    )
    out_specs = P("expert", TP)
    return jax.shard_map(local, mesh=split, in_specs=in_specs, out_specs=out_specs, check_vma=False)
```
